256 devices in a mesh: px: 16 (over x_hi, z), py: 16 (over y, x_lo, core).
Axes of the slice: x: 4 (x_hi: 2, x_lo: 2; x = x_hi * 2 + x_lo), y: 4, z: 8, core: 2. Of those that a mesh axis runs over, the one named last changes fastest.
Arguments:
- particles: float32 [256, 2, 2, 128, 128], P(('px', 'py')), may hold values from -11 to 11
- orientation: int32 [256], P(('px', 'py')), may hold values from 0 to 7
- wedge_index: int32 [256], P(('px', 'py')), may hold values from 0 to 3
- half_set: int32 [256], P(('px', 'py')), may hold values from 0 to 1
- shell_map: int32 [2, 256, 256], P(None, ('px', 'py')), may hold values from 0 to 31, as said below
Outputs:
- half_maps: float32 [2, 2, 2, 256, 256], P(None, None, None, ('px', 'py'))
- fsc: float32 [32], replicated
The draws below stay inside these ranges and needn't reach their ends.
Inputs may be any that keep to these rules, and one draw needn't show every extreme that they name: `shell_map`: every shell number occurs in every draw.
All inputs are finite; a program needn't handle non-finite values.
Results may differ from the reference program's by a relative error of at most 0.0003.
Values sent between devices are 32-bit elements; how exact they have to be, the bound alone decides.
A program may use at most 64 MiB of HBM per device.

```python
import functools
import jax
import jax.numpy as jnp
from jax import lax

N = 256
BOX = 128
NZ = 2
NSHELL = 32
PARTICLES = 256


def draw_particles(key, part):
    full_shape = (PARTICLES, 2, NZ, BOX, BOX)
    common = 0.8 * jnp.clip(jax.random.normal(jax.random.fold_in(key, 11), full_shape[1:], jnp.float32), -6.0, 6.0)
    noise = jnp.clip(jax.random.normal(jax.random.fold_in(key, 12), full_shape, jnp.float32), -6.0, 6.0)
    return common[None] + noise


def draw_shell_map(key, part):
    weights_axis = jax.random.randint(jax.random.fold_in(key, 21), (3,), 4, 10, dtype=jnp.int32)
    spectral = jnp.arange(N, dtype=jnp.int32)
    signed = jnp.where(spectral < N // 2, spectral, spectral - N)
    planes = (jnp.arange(NZ, dtype=jnp.int32) - NZ // 2) * (N // NZ)
    radius_sq = weights_axis[2] * planes[:, None, None] ** 2 + weights_axis[0] * signed[None, :, None] ** 2 + weights_axis[1] * signed[None, None, :] ** 2
    spacing = N // NSHELL
    bounds = (jnp.arange(1, NSHELL, dtype=jnp.int32) * spacing) ** 2
    return jnp.sum((radius_sq[..., None] >= bounds).astype(jnp.int32), axis=-1)


def touch_ends(result, stream_key, smallest, high):
    extent = result.shape
    place = [jax.random.randint(jax.random.fold_in(stream_key, axis), (), 0, extent[axis]) for axis in range(len(extent))]
    result = result.at[tuple(place)].set(smallest)
    longest = extent.index(max(extent))
    place[longest] = (place[longest] + 1) % extent[longest]
    return result.at[tuple(place)].set(high)


def setup_inputs(seed: int = 0) -> dict:
    arg_keys = jax.random.split(jax.random.key(seed), 6)
    return {
        "particles": draw_particles(jax.random.fold_in(arg_keys[5], 71), 0),
        "orientation": touch_ends(jax.random.randint(arg_keys[1], (PARTICLES,), 0, 8), jax.random.fold_in(arg_keys[1], 1), 0, 7).astype(jnp.int32),
        "wedge_index": touch_ends(jax.random.randint(arg_keys[2], (PARTICLES,), 0, 4), jax.random.fold_in(arg_keys[2], 1), 0, 3).astype(jnp.int32),
        "half_set": touch_ends(jax.random.randint(arg_keys[3], (PARTICLES,), 0, 2), jax.random.fold_in(arg_keys[3], 1), 0, 1).astype(jnp.int32),
        "shell_map": draw_shell_map(jax.random.fold_in(arg_keys[5], 71), 0),
    }


wedge_rise = (1, 3, 2, 3)
wedge_run = (1, 2, 1, 1)

def negate(values, dimension):
    return jnp.roll(jnp.flip(values, dimension), 1, dimension)

def quarter(values):
    return jnp.swapaxes(negate(values, -1), -1, -2)

def orient_branch(values, turns, mirror):
    for repeat in range(turns):
        values = quarter(values)
    if mirror:
        values = negate(negate(values, -3), -1)
    return values

def reference(particles, orientation, wedge_index, half_set, shell_map):
    plane_abs = jnp.abs((jnp.arange(NZ, dtype=jnp.int32) - NZ // 2) * (N // NZ))
    spectral = jnp.arange(N, dtype=jnp.int32)
    spectral_abs = jnp.minimum(spectral, N - spectral)
    rise_table = jnp.array(wedge_rise, dtype=jnp.int32)
    run_table = jnp.array(wedge_run, dtype=jnp.int32)
    branches = [functools.partial(orient_branch, turns=code % 4, mirror=code >= 4) for code in range(8)]

    def accumulate(carry, item):
        totals, cover_sum = carry
        source, turn_index, wedge_id, half_id = item
        padded = jnp.zeros((2, NZ, N, N), jnp.float32).at[:, :, :BOX, :BOX].set(source)
        padded = jnp.roll(padded, (-(BOX // 2), -(BOX // 2)), axis=(2, 3))
        spectrum = jnp.fft.fft2(padded[0] + 1j * padded[1], norm='ortho')
        covered = (plane_abs[:, None] * run_table[wedge_id] <= spectral_abs[None, :] * rise_table[wedge_id]).astype(jnp.float32)
        covered = jnp.broadcast_to(covered[:, :, None], (NZ, N, N))
        stacked = jnp.stack([jnp.real(spectrum) * covered, jnp.imag(spectrum) * covered, covered])
        turned = lax.switch(turn_index, branches, stacked)
        totals = totals.at[half_id].add(turned[:2])
        cover_sum = cover_sum.at[half_id].add(turned[2])
        return ((totals, cover_sum), None)
    start = (jnp.zeros((2, 2, NZ, N, N), jnp.float32), jnp.zeros((2, NZ, N, N), jnp.float32))
    (totals, cover_sum), unused = lax.scan(accumulate, start, (particles, orientation, wedge_index, half_set))
    average = totals / jnp.maximum(cover_sum, 1.0)[:, None]
    cross = average[0, 0] * average[1, 0] + average[0, 1] * average[1, 1]
    power_first = average[0, 0] * average[0, 0] + average[0, 1] * average[0, 1]
    power_second = average[1, 0] * average[1, 0] + average[1, 1] * average[1, 1]
    labels = shell_map.reshape(-1)
    cross_sum = jax.ops.segment_sum(cross.reshape(-1), labels, num_segments=NSHELL)
    first_sum = jax.ops.segment_sum(power_first.reshape(-1), labels, num_segments=NSHELL)
    second_sum = jax.ops.segment_sum(power_second.reshape(-1), labels, num_segments=NSHELL)
    fsc = cross_sum / (jnp.sqrt(first_sum * second_sum) + 1e-06)
    spatial = jnp.fft.ifft2(average[:, 0] + 1j * average[:, 1], norm='ortho')
    half_maps = jnp.stack([jnp.real(spatial), jnp.imag(spatial)], axis=1)
    half_maps = jnp.swapaxes(half_maps, -1, -2)
    return (half_maps, fsc)
```

```python
import functools
import math

import jax
import jax.numpy as jnp
import numpy as np
from jax import lax
from jax.experimental import pallas as pl
from jax.experimental.pallas import tpu as pltpu
from jax.sharding import PartitionSpec as P

RISE = (1, 3, 2, 3)
RUN = (1, 2, 1, 1)
NSHELL = 32
SIDE = 16
EXTENT = 256
BOX = 128
KZ = 128
THRESHOLDS = tuple(-(-KZ * run // rise) for rise, run in zip(RISE, RUN))
MESH = pl.DeviceIdType.MESH
f32 = jnp.float32
bf16 = jnp.bfloat16
NT = (((1,), (1,)), ((), ()))
NN = (((1,), (0,)), ((), ()))
MAPLANE = 96


def halves(table):
    table = jnp.asarray(table, f32)
    upper = table.astype(bf16)
    lower = (table - upper.astype(f32)).astype(bf16)
    return jnp.stack([upper, lower])


def tables():
    freq = np.arange(EXTENT)
    cell = np.arange(BOX) - BOX // 2
    scale = 1.0 / math.sqrt(EXTENT)
    unit = 2.0 * math.pi / EXTENT
    rows = np.arange(SIDE)
    order = (rows[None, :] * SIDE + rows[:, None]).reshape(-1)
    angle = (order[:, None] * cell[None, :] % EXTENT) * unit
    first = np.concatenate([np.cos(angle), np.sin(angle)], 1) * scale
    angle = (cell[:, None] * freq[None, :] % EXTENT) * unit
    cosine, sine = np.cos(angle) * scale, np.sin(angle) * scale
    second = np.block([[cosine, -sine], [sine, cosine]])
    angle = (freq[:, None] * freq[None, :] % EXTENT) * unit
    back = np.concatenate([np.cos(angle), np.sin(angle)], 1) * scale
    return [np.asarray(t, np.float32) for t in (first, second, back)]


def cut(value):
    upper = value.astype(bf16)
    return upper, (value - upper.astype(f32)).astype(bf16)


def dot(a, b, dims):
    return lax.dot_general(a, b, dims, preferred_element_type=f32)


def dot3(a, b, dims):
    return dot(a[0], b[0], dims) + (dot(a[0], b[1], dims) + dot(a[1], b[0], dims))


def magnitude(index):
    return jnp.minimum(index, EXTENT - index)


def pick(position, entries):
    result = jnp.full_like(position, entries[0])
    for number, entry in enumerate(entries[1:], 1):
        result = jnp.where(position == number, entry, result)
    return result


def quarter_phase(value):
    row = lax.broadcasted_iota(jnp.int32, value.shape, 0)
    return jnp.where(row // 2 % 2 == 0, -pltpu.roll(value, 6, 0), pltpu.roll(value, 2, 0))


def body(
    orient, wedge, half, particle, shell, first_t, second_t, back_t, maps_ref, fsc_ref,
    source, first, second, back, slab_out, slab_in, tag_out, tag_in,
    sum_out, sum_in, count_out, count_in, row_out, row_in,
    load_sem, slab_s, slab_r, tag_s, tag_r, sum_s, sum_r, count_s, count_r, row_s, row_r,
):
    px, py = lax.axis_index("px"), lax.axis_index("py")
    me = px * SIDE + py
    loads = [
        pltpu.make_async_copy(a, b, load_sem.at[i])
        for i, (a, b) in enumerate(
            [(particle, source), (first_t, first), (second_t, second), (back_t, back)]
        )
    ]
    for load in loads:
        load.start()
    barrier = pltpu.get_barrier_semaphore()
    for k in range(1, SIDE):
        pl.semaphore_signal(
            barrier, 1, device_id=(px, lax.rem(py + k, SIDE)), device_id_type=MESH
        )
        pl.semaphore_signal(
            barrier, 1, device_id=(lax.rem(px + k, SIDE), py), device_id_type=MESH
        )

    turn, wedge_id, half_id = orient[0], wedge[0], half[0]
    quarter = turn % 4
    sign_x = (1 - 2 * ((quarter + 1) // 2 % 2)).astype(f32)
    sign_y = ((1 - 2 * (quarter // 2)) * (1 - 2 * (turn // 4))).astype(f32)
    swapped = turn % 2

    tag_row = lax.broadcasted_iota(jnp.int32, (4, 128), 0)
    tag_lane = lax.broadcasted_iota(jnp.int32, (4, 128), 1)
    limit = pick(jnp.broadcast_to(wedge_id, (4, 128)), THRESHOLDS) * swapped
    own_class = half_id * 8 + swapped * 4 + wedge_id
    tag = jnp.where(tag_row == 0, limit.astype(f32), 0.0)
    tag = jnp.where(tag_row == 1, jnp.broadcast_to(half_id, (4, 128)).astype(f32), tag)
    tag = jnp.where(tag_row == 2, jnp.broadcast_to(sign_y, (4, 128)), tag)
    tag = jnp.where(tag_row == 3, jnp.where(tag_lane == own_class, 1.0, 0.0), tag)
    tag_out[...] = tag
    tag_in[py] = tag

    row = lax.broadcasted_iota(jnp.int32, (EXTENT, EXTENT), 0)
    kx_abs = magnitude(row % SIDE * SIDE + row // SIDE)
    row_limit = pick(jnp.broadcast_to(wedge_id, (EXTENT, EXTENT)), THRESHOLDS) * (1 - swapped)
    row_mask = jnp.where(kx_abs >= row_limit, 1.0, 0.0)
    turned = jnp.broadcast_to(swapped, (BOX, BOX)) == 1
    loads[0].wait()
    loads[1].wait()
    for z in range(2):
        real, imag = source[0, z], source[1, z]
        real = jnp.where(turned, real.T, real)
        imag = jnp.where(turned, imag.T, imag)
        stacked = jnp.concatenate(
            [
                jnp.concatenate([real, imag * sign_y], 1),
                jnp.concatenate([imag * sign_x, real * (-sign_x * sign_y)], 1),
            ],
            0,
        )
        along = dot3((first[0], first[1]), cut(stacked), NN)
        if z == 0:
            along = along * row_mask
        slab_out[:, z * SIDE : (z + 1) * SIDE, :] = along.reshape(SIDE, SIDE, EXTENT)
    slab_in[py] = slab_out[py]
    pl.semaphore_wait(barrier, 2 * (SIDE - 1))

    sent = []
    for k in range(1, SIDE):
        other = lax.rem(py + k, SIDE)
        sent.append(
            pltpu.make_async_remote_copy(
                tag_out, tag_in.at[py], tag_s.at[k], tag_r.at[k], (px, other), MESH
            )
        )
        sent.append(
            pltpu.make_async_remote_copy(
                slab_out.at[other], slab_in.at[py], slab_s.at[k], slab_r.at[k], (px, other), MESH
            )
        )
    for copy in sent:
        copy.start()
    loads[2].wait()
    for copy in sent:
        copy.wait_recv()

    ky = lax.broadcasted_iota(jnp.int32, (1, EXTENT), 1)
    ky_abs = magnitude(ky).astype(f32)
    second_pair = (second[0], second[1])
    totals = [[jnp.zeros((SIDE, 2 * EXTENT), f32) for z in range(2)] for h in range(2)]
    counts = jnp.zeros((1, 128), f32)
    group = 4
    for start in range(0, SIDE, group):
        block = slab_in[start : start + group].reshape(group * 2 * SIDE, EXTENT)
        spread = dot3(cut(block), second_pair, NN)
        for g in range(group):
            tag = tag_in[start + g]
            lane_limit = jnp.concatenate([tag[0:1], tag[0:1]], 1)
            lane_half = jnp.concatenate([tag[1:2]] * 4, 1)
            lane_sign = jnp.concatenate([tag[2:3], tag[2:3]], 1)
            keep = jnp.where(ky_abs >= lane_limit, 1.0, 0.0)
            factors = (
                jnp.concatenate([keep, keep * lane_sign], 1),
                jnp.concatenate([jnp.ones_like(keep), lane_sign], 1),
            )
            counts = counts + tag[3:4]
            for z in range(2):
                base = (g * 2 + z) * SIDE
                value = spread[base : base + SIDE] * factors[z]
                upper = value * lane_half
                totals[1][z] = totals[1][z] + upper
                totals[0][z] = totals[0][z] + (value - upper)
    for h in range(2):
        for c in range(2):
            for z in range(2):
                sum_out[:, h * 4 + c * 2 + z, :] = totals[h][z][:, c * EXTENT : (c + 1) * EXTENT]
    count_out[...] = counts
    count_in[px] = counts
    sum_in[px] = sum_out[px]

    summed = []
    for k in range(1, SIDE):
        other = lax.rem(px + k, SIDE)
        summed.append(
            pltpu.make_async_remote_copy(
                count_out, count_in.at[px], count_s.at[k], count_r.at[k], (other, py), MESH
            )
        )
        summed.append(
            pltpu.make_async_remote_copy(
                sum_out.at[other], sum_in.at[px], sum_s.at[k], sum_r.at[k], (other, py), MESH
            )
        )
    for copy in summed:
        copy.start()
    loads[3].wait()

    comp = lax.broadcasted_iota(jnp.int32, (8, 128), 0)
    lane = lax.broadcasted_iota(jnp.int32, (8, 128), 1)
    kind = lax.broadcasted_iota(jnp.int32, (128, EXTENT), 0)
    ky_wide = magnitude(lax.broadcasted_iota(jnp.int32, (128, EXTENT), 1))
    reach = jnp.where(kind // 4 % 2 == 1, ky_wide, magnitude(me))
    inside = jnp.where(reach >= pick(kind % 4, THRESHOLDS), 1.0, 0.0).astype(bf16)
    number = lax.broadcasted_iota(jnp.int32, (128, EXTENT), 0) % NSHELL
    members = [jnp.where(number == shell[z], 1.0, 0.0).astype(bf16) for z in range(2)]
    for copy in summed:
        copy.wait_recv()
    total = sum_in[0]
    count = count_in[0]
    for k in range(1, SIDE):
        total = total + sum_in[k]
        count = count + count_in[k]
    by_half = jnp.where(lane // 8 == comp // 4, count, 0.0)
    masked_count = dot(by_half.astype(bf16), inside, NN)
    full_count = jnp.sum(by_half, axis=1, keepdims=True)
    wide_comp = lax.broadcasted_iota(jnp.int32, (8, EXTENT), 0)
    cover = jnp.where(wide_comp % 2 == 0, masked_count, full_count)
    average = total / jnp.maximum(cover, 1.0)

    powers = jnp.concatenate([average * average, average * pltpu.roll(average, 4, 0)], 0)
    powers = cut(powers)
    p_row = lax.broadcasted_iota(jnp.int32, (16, 128), 0)
    p_lane = lax.broadcasted_iota(jnp.int32, (16, 128), 1)
    wanted = jnp.where(p_row < 8, 1 + p_row // 4, jnp.where(p_row < 12, 0, 4))
    shells = jnp.zeros((1, 128), f32)
    for z in range(2):
        part = dot(powers[0], members[z], NT) + dot(powers[1], members[z], NT)
        part = jnp.where((p_row % 2 == z) & (p_lane // NSHELL == wanted), part, 0.0)
        shells = shells + jnp.sum(part, axis=0, keepdims=True)

    back_pair = (back[0], back[1])
    pair = jnp.concatenate([average, quarter_phase(average)], 1)
    padded = jnp.concatenate(
        [
            jnp.zeros((MAPLANE, 2 * EXTENT), f32),
            pair,
            jnp.zeros((128 - MAPLANE - 8, 2 * EXTENT), f32),
        ],
        0,
    )
    middle = dot3(back_pair, cut(padded), NT)
    row_out[...] = (middle + shells).reshape(EXTENT, 1, 128)
    row_in[me] = row_out[me]

    @pl.loop(1, EXTENT)
    def _(k):
        other = lax.rem(me + k, EXTENT)
        pltpu.make_async_remote_copy(
            row_out.at[other], row_in.at[me], row_s, row_r, (other // SIDE, other % SIDE), MESH
        ).start()

    whole = row_in.at[pl.ds(0, EXTENT - 1)]
    pltpu.make_async_copy(whole, whole, row_r).wait()
    rows = row_in[...].reshape(EXTENT, 128)
    sums = jnp.sum(rows, axis=0, keepdims=True)
    values = rows.T[MAPLANE : MAPLANE + 8]
    pair = jnp.concatenate([values, quarter_phase(values)], 1)
    final = dot3(cut(pair), back_pair, NT)
    for h in range(2):
        for c in range(2):
            for z in range(2):
                n = h * 4 + c * 2 + z
                maps_ref[h, c, z] = final[n : n + 1]
    sums = jnp.broadcast_to(sums, (8, 128))
    first_power = pltpu.roll(sums, 128 - NSHELL, 1)
    second_power = pltpu.roll(sums, 128 - 2 * NSHELL, 1)
    fsc_ref[...] = sums / (jnp.sqrt(first_power * second_power) + 1e-06)

    for copy in sent + summed:
        copy.wait_send()
    pltpu.make_async_copy(whole, whole, row_s).wait()


def shards(particles, orientation, wedge_index, half_set, shell_map):
    first, second, back = (halves(t) for t in tables())
    smem = pl.BlockSpec(memory_space=pltpu.SMEM)
    vmem = pl.BlockSpec(memory_space=pltpu.VMEM)
    hbm = pl.BlockSpec(memory_space=pl.ANY)
    dma = pltpu.SemaphoreType.DMA
    maps, fsc = pl.pallas_call(
        body,
        out_shape=(
            jax.ShapeDtypeStruct((2, 2, 2, 1, EXTENT), f32),
            jax.ShapeDtypeStruct((8, 128), f32),
        ),
        in_specs=[smem, smem, smem, hbm, vmem, hbm, hbm, hbm],
        out_specs=(vmem, vmem),
        scratch_shapes=[
            pltpu.VMEM((2, 2, BOX, BOX), f32),
            pltpu.VMEM((2, EXTENT, EXTENT), bf16),
            pltpu.VMEM((2, EXTENT, 2 * EXTENT), bf16),
            pltpu.VMEM((2, EXTENT, 2 * EXTENT), bf16),
            pltpu.VMEM((SIDE, 2 * SIDE, EXTENT), f32),
            pltpu.VMEM((SIDE, 2 * SIDE, EXTENT), f32),
            pltpu.VMEM((4, 128), f32),
            pltpu.VMEM((SIDE, 4, 128), f32),
            pltpu.VMEM((SIDE, 8, EXTENT), f32),
            pltpu.VMEM((SIDE, 8, EXTENT), f32),
            pltpu.VMEM((1, 128), f32),
            pltpu.VMEM((SIDE, 1, 128), f32),
            pltpu.VMEM((EXTENT, 1, 128), f32),
            pltpu.VMEM((EXTENT, 1, 128), f32),
            dma((4,)),
            dma((SIDE,)), dma((SIDE,)), dma((SIDE,)), dma((SIDE,)),
            dma((SIDE,)), dma((SIDE,)), dma((SIDE,)), dma((SIDE,)),
            dma, dma,
        ],
        compiler_params=pltpu.CompilerParams(collective_id=0, has_side_effects=True),
        name="subtomogram_average",
    )(orientation, wedge_index, half_set, particles[0], shell_map, first, second, back)
    return maps, fsc[0, :NSHELL]


def solution(mesh):
    both = ("px", "py")
    return jax.shard_map(
        shards,
        mesh=mesh,
        in_specs=(P(both, None, None, None, None), P(both), P(both), P(both), P(None, both, None)),
        out_specs=(P(None, None, None, both, None), P()),
        check_vma=False,
    )
```

```python
import functools
import math

import jax
import jax.numpy as jnp
import numpy as np
from jax import lax
from jax.experimental import pallas as pl
from jax.experimental.pallas import tpu as pltpu
from jax.sharding import PartitionSpec as P

RISE = (1, 3, 2, 3)
RUN = (1, 2, 1, 1)
NSHELL = 32
PLANE = 32
DEPTH = 8
LINE = 16
EXTENT = 256
BOX = 128
KZ = 128
THRESHOLDS = tuple(-(-KZ * run // rise) for rise, run in zip(RISE, RUN))
MESH = pl.DeviceIdType.MESH
f32 = jnp.float32
bf16 = jnp.bfloat16
NT = (((1,), (1,)), ((), ()))
NN = (((1,), (0,)), ((), ()))
MAPLANE = 96


def halves(table):
    table = jnp.asarray(table, f32)
    upper = table.astype(bf16)
    lower = (table - upper.astype(f32)).astype(bf16)
    return jnp.stack([upper, lower])


def tables():
    freq = np.arange(EXTENT)
    cell = np.arange(BOX) - BOX // 2
    scale = 1.0 / math.sqrt(EXTENT)
    unit = 2.0 * math.pi / EXTENT
    place, level = np.arange(PLANE)[:, None], np.arange(DEPTH)[None, :]
    order = (place // LINE * (LINE * DEPTH) + level * LINE + place % LINE).reshape(-1)
    angle = (order[:, None] * cell[None, :] % EXTENT) * unit
    first = np.concatenate([np.cos(angle), np.sin(angle)], 1) * scale
    angle = (cell[:, None] * freq[None, :] % EXTENT) * unit
    cosine, sine = np.cos(angle) * scale, np.sin(angle) * scale
    second = np.block([[cosine, -sine], [sine, cosine]])
    angle = (freq[:, None] * freq[None, :] % EXTENT) * unit
    back = np.concatenate([np.cos(angle), np.sin(angle)], 1) * scale
    return [np.asarray(t, np.float32) for t in (first, second, back)]


def cut(value):
    upper = value.astype(bf16)
    return upper, (value - upper.astype(f32)).astype(bf16)


def dot(a, b, dims):
    return lax.dot_general(a, b, dims, preferred_element_type=f32)


def dot3(a, b, dims):
    return dot(a[0], b[0], dims) + (dot(a[0], b[1], dims) + dot(a[1], b[0], dims))


def magnitude(index):
    return jnp.minimum(index, EXTENT - index)


def pick(position, entries):
    result = jnp.full_like(position, entries[0])
    for number, entry in enumerate(entries[1:], 1):
        result = jnp.where(position == number, entry, result)
    return result


def quarter_phase(value):
    row = lax.broadcasted_iota(jnp.int32, value.shape, 0)
    return jnp.where(row // 2 % 2 == 0, -pltpu.roll(value, 6, 0), pltpu.roll(value, 2, 0))


def body(
    orient, wedge, half, particle, shell, first_t, second_t, back_t, maps_ref, fsc_ref,
    source, first, second, back, slab_out, slab_in, tag_out, tag_in,
    sum_out, sum_in, count_out, count_in, row_out, row_in,
    load_sem, slab_s, slab_r, tag_s, tag_r, sum_s, sum_r, count_s, count_r, row_s, row_r,
    above_sem, below_sem,
):
    px, py = lax.axis_index("px"), lax.axis_index("py")
    me = px * LINE + py
    side, level = lax.div(px, DEPTH), lax.rem(px, DEPTH)
    place = side * LINE + py
    sides = [side, 1 - side]
    lines = [py] + [lax.rem(py + b, LINE) for b in range(1, LINE)]
    far_first = [8, 9, 10, 11, 7, 6, 5, 4, 12, 13, 14, 15, 3, 2, 1, 0]
    plane = [(sides[a], lines[b]) for b in far_first for a in (1, 0)][:-1]
    levels = [level] + [lax.rem(level + c, DEPTH) for c in range(1, DEPTH)]
    column = [levels[c] for c in (4, 3, 5, 2, 6, 1, 7)]
    above = (side * DEPTH + levels[1], py)
    below = (side * DEPTH + levels[7], py)
    loads = [
        pltpu.make_async_copy(a, b, load_sem.at[i])
        for i, (a, b) in enumerate(
            [(particle, source), (first_t, first), (second_t, second), (back_t, back)]
        )
    ]
    for load in loads:
        load.start()
    barrier = pltpu.get_barrier_semaphore()
    for a, b in plane:
        pl.semaphore_signal(barrier, 1, device_id=(a * DEPTH + level, b), device_id_type=MESH)
    for neighbour in (above, below):
        pl.semaphore_signal(barrier, 1, device_id=neighbour, device_id_type=MESH)

    turn, wedge_id, half_id = orient[0], wedge[0], half[0]
    quarter = turn % 4
    sign_x = (1 - 2 * ((quarter + 1) // 2 % 2)).astype(f32)
    sign_y = ((1 - 2 * (quarter // 2)) * (1 - 2 * (turn // 4))).astype(f32)
    swapped = turn % 2

    tag_row = lax.broadcasted_iota(jnp.int32, (4, 128), 0)
    tag_lane = lax.broadcasted_iota(jnp.int32, (4, 128), 1)
    limit = pick(jnp.broadcast_to(wedge_id, (4, 128)), THRESHOLDS) * swapped
    own_class = half_id * 8 + swapped * 4 + wedge_id
    tag = jnp.where(tag_row == 0, limit.astype(f32), 0.0)
    tag = jnp.where(tag_row == 1, jnp.broadcast_to(half_id, (4, 128)).astype(f32), tag)
    tag = jnp.where(tag_row == 2, jnp.broadcast_to(sign_y, (4, 128)), tag)
    tag = jnp.where(tag_row == 3, jnp.where(tag_lane == own_class, 1.0, 0.0), tag)
    tag_out[...] = tag
    tag_in[place] = tag

    row = lax.broadcasted_iota(jnp.int32, (EXTENT, EXTENT), 0)
    kx = row // (DEPTH * LINE) * (DEPTH * LINE) + row % DEPTH * LINE + row // DEPTH % LINE
    kx_abs = magnitude(kx)
    row_limit = pick(jnp.broadcast_to(wedge_id, (EXTENT, EXTENT)), THRESHOLDS) * (1 - swapped)
    row_mask = jnp.where(kx_abs >= row_limit, 1.0, 0.0)
    turned = jnp.broadcast_to(swapped, (BOX, BOX)) == 1
    loads[0].wait()
    loads[1].wait()
    for z in range(2):
        real, imag = source[0, z], source[1, z]
        real = jnp.where(turned, real.T, real)
        imag = jnp.where(turned, imag.T, imag)
        stacked = jnp.concatenate(
            [
                jnp.concatenate([real, imag * sign_y], 1),
                jnp.concatenate([imag * sign_x, real * (-sign_x * sign_y)], 1),
            ],
            0,
        )
        along = dot3((first[0], first[1]), cut(stacked), NN)
        if z == 0:
            along = along * row_mask
        slab_out[:, z * DEPTH : (z + 1) * DEPTH, :] = along.reshape(PLANE, DEPTH, EXTENT)
    slab_in[place] = slab_out[place]
    pl.semaphore_wait(barrier, PLANE + 1)

    sent = []
    for k, (a, b) in enumerate(plane):
        to = (a * DEPTH + level, b)
        sent.append(
            pltpu.make_async_remote_copy(
                tag_out, tag_in.at[place], tag_s.at[k], tag_r.at[k], to, MESH
            )
        )
        sent.append(
            pltpu.make_async_remote_copy(
                slab_out.at[a * LINE + b], slab_in.at[place], slab_s.at[k], slab_r.at[k], to, MESH
            )
        )
    for copy in sent:
        copy.start()
    for step in range(3):
        pl.semaphore_signal(above_sem.at[step], 1, device_id=above, device_id_type=MESH)
        if step < 2:
            pl.semaphore_signal(below_sem.at[step], 1, device_id=below, device_id_type=MESH)
            pl.semaphore_wait(below_sem.at[step], 1)
        pl.semaphore_wait(above_sem.at[step], 1)
    loads[2].wait()
    for copy in sent:
        copy.wait_recv()

    ky = lax.broadcasted_iota(jnp.int32, (1, EXTENT), 1)
    ky_abs = magnitude(ky).astype(f32)
    second_pair = (second[0], second[1])
    totals = [[jnp.zeros((DEPTH, 2 * EXTENT), f32) for z in range(2)] for h in range(2)]
    counts = jnp.zeros((1, 128), f32)
    group = 8
    for start in range(0, PLANE, group):
        block = slab_in[start : start + group].reshape(group * 2 * DEPTH, EXTENT)
        spread = dot3(cut(block), second_pair, NN)
        for g in range(group):
            tag = tag_in[start + g]
            lane_limit = jnp.concatenate([tag[0:1], tag[0:1]], 1)
            lane_half = jnp.concatenate([tag[1:2]] * 4, 1)
            lane_sign = jnp.concatenate([tag[2:3], tag[2:3]], 1)
            keep = jnp.where(ky_abs >= lane_limit, 1.0, 0.0)
            factors = (
                jnp.concatenate([keep, keep * lane_sign], 1),
                jnp.concatenate([jnp.ones_like(keep), lane_sign], 1),
            )
            counts = counts + tag[3:4]
            for z in range(2):
                base = (g * 2 + z) * DEPTH
                value = spread[base : base + DEPTH] * factors[z]
                upper = value * lane_half
                totals[1][z] = totals[1][z] + upper
                totals[0][z] = totals[0][z] + (value - upper)
    for h in range(2):
        for c in range(2):
            for z in range(2):
                sum_out[:, h * 4 + c * 2 + z, :] = totals[h][z][:, c * EXTENT : (c + 1) * EXTENT]
    count_out[...] = counts
    count_in[level] = counts
    sum_in[level] = sum_out[level]

    summed = []
    for k, other in enumerate(column):
        to = (side * DEPTH + other, py)
        summed.append(
            pltpu.make_async_remote_copy(
                count_out, count_in.at[level], count_s.at[k], count_r.at[k], to, MESH
            )
        )
        summed.append(
            pltpu.make_async_remote_copy(
                sum_out.at[other], sum_in.at[level], sum_s.at[k], sum_r.at[k], to, MESH
            )
        )
    for copy in summed:
        copy.start()
    loads[3].wait()

    comp = lax.broadcasted_iota(jnp.int32, (8, 128), 0)
    lane = lax.broadcasted_iota(jnp.int32, (8, 128), 1)
    kind = lax.broadcasted_iota(jnp.int32, (128, EXTENT), 0)
    ky_wide = magnitude(lax.broadcasted_iota(jnp.int32, (128, EXTENT), 1))
    reach = jnp.where(kind // 4 % 2 == 1, ky_wide, magnitude(me))
    inside = jnp.where(reach >= pick(kind % 4, THRESHOLDS), 1.0, 0.0).astype(bf16)
    number = lax.broadcasted_iota(jnp.int32, (128, EXTENT), 0) % NSHELL
    members = [jnp.where(number == shell[z], 1.0, 0.0).astype(bf16) for z in range(2)]
    for copy in summed:
        copy.wait_recv()
    total = sum_in[0]
    count = count_in[0]
    for k in range(1, DEPTH):
        total = total + sum_in[k]
        count = count + count_in[k]
    by_half = jnp.where(lane // 8 == comp // 4, count, 0.0)
    masked_count = dot(by_half.astype(bf16), inside, NN)
    full_count = jnp.sum(by_half, axis=1, keepdims=True)
    wide_comp = lax.broadcasted_iota(jnp.int32, (8, EXTENT), 0)
    cover = jnp.where(wide_comp % 2 == 0, masked_count, full_count)
    average = total / jnp.maximum(cover, 1.0)

    powers = jnp.concatenate([average * average, average * pltpu.roll(average, 4, 0)], 0)
    powers = cut(powers)
    p_row = lax.broadcasted_iota(jnp.int32, (16, 128), 0)
    p_lane = lax.broadcasted_iota(jnp.int32, (16, 128), 1)
    wanted = jnp.where(p_row < 8, 1 + p_row // 4, jnp.where(p_row < 12, 0, 4))
    shells = jnp.zeros((1, 128), f32)
    for z in range(2):
        part = dot(powers[0], members[z], NT) + dot(powers[1], members[z], NT)
        part = jnp.where((p_row % 2 == z) & (p_lane // NSHELL == wanted), part, 0.0)
        shells = shells + jnp.sum(part, axis=0, keepdims=True)

    back_pair = (back[0], back[1])
    pair = jnp.concatenate([average, quarter_phase(average)], 1)
    padded = jnp.concatenate(
        [
            jnp.zeros((MAPLANE, 2 * EXTENT), f32),
            pair,
            jnp.zeros((128 - MAPLANE - 8, 2 * EXTENT), f32),
        ],
        0,
    )
    middle = dot3(back_pair, cut(padded), NT)
    row_out[...] = middle + shells
    row_in[pl.ds(me, 1)] = row_out[pl.ds(me, 1)]

    def send_row(a, c, b):
        to = (a * DEPTH + c, b)
        other = to[0] * LINE + b
        pltpu.make_async_remote_copy(
            row_out.at[pl.ds(other, 1)], row_in.at[pl.ds(me, 1)], row_s, row_r, to, MESH
        ).start()

    @pl.loop(0, DEPTH - 1)
    def _(step):
        away = lax.div(step + 1, 2)
        shift = away * (1 - 2 * lax.rem(step, 2))
        other = lax.rem(level + 12 + shift, DEPTH)
        for a, b in plane + [(side, py)]:
            send_row(a, other, b)

    for a, b in plane:
        send_row(a, level, b)

    whole = row_in.at[pl.ds(0, EXTENT - 1)]
    pltpu.make_async_copy(whole, whole, row_r).wait()
    rows = row_in[...]
    sums = jnp.sum(rows, axis=0, keepdims=True)
    values = rows.T[MAPLANE : MAPLANE + 8]
    pair = jnp.concatenate([values, quarter_phase(values)], 1)
    final = dot3(cut(pair), back_pair, NT)
    for h in range(2):
        for c in range(2):
            for z in range(2):
                n = h * 4 + c * 2 + z
                maps_ref[h, c, z] = final[n : n + 1]
    sums = jnp.broadcast_to(sums, (8, 128))
    first_power = pltpu.roll(sums, 128 - NSHELL, 1)
    second_power = pltpu.roll(sums, 128 - 2 * NSHELL, 1)
    fsc_ref[...] = sums / (jnp.sqrt(first_power * second_power) + 1e-06)

    for copy in sent + summed:
        copy.wait_send()
    pltpu.make_async_copy(whole, whole, row_s).wait()


def shards(particles, orientation, wedge_index, half_set, shell_map):
    first, second, back = (halves(t) for t in tables())
    smem = pl.BlockSpec(memory_space=pltpu.SMEM)
    vmem = pl.BlockSpec(memory_space=pltpu.VMEM)
    hbm = pl.BlockSpec(memory_space=pl.ANY)
    dma = pltpu.SemaphoreType.DMA
    maps, fsc = pl.pallas_call(
        body,
        out_shape=(
            jax.ShapeDtypeStruct((2, 2, 2, 1, EXTENT), f32),
            jax.ShapeDtypeStruct((8, 128), f32),
        ),
        in_specs=[smem, smem, smem, hbm, vmem, hbm, hbm, hbm],
        out_specs=(vmem, vmem),
        scratch_shapes=[
            pltpu.VMEM((2, 2, BOX, BOX), f32),
            pltpu.VMEM((2, EXTENT, EXTENT), bf16),
            pltpu.VMEM((2, EXTENT, 2 * EXTENT), bf16),
            pltpu.VMEM((2, EXTENT, 2 * EXTENT), bf16),
            pltpu.VMEM((PLANE, 2 * DEPTH, EXTENT), f32),
            pltpu.VMEM((PLANE, 2 * DEPTH, EXTENT), f32),
            pltpu.VMEM((4, 128), f32),
            pltpu.VMEM((PLANE, 4, 128), f32),
            pltpu.VMEM((DEPTH, 8, EXTENT), f32),
            pltpu.VMEM((DEPTH, 8, EXTENT), f32),
            pltpu.VMEM((1, 128), f32),
            pltpu.VMEM((DEPTH, 1, 128), f32),
            pltpu.VMEM((EXTENT, 128), f32),
            pltpu.VMEM((EXTENT, 128), f32),
            dma((4,)),
            dma((PLANE,)), dma((PLANE,)), dma((PLANE,)), dma((PLANE,)),
            dma((DEPTH,)), dma((DEPTH,)), dma((DEPTH,)), dma((DEPTH,)),
            dma, dma,
            pltpu.SemaphoreType.REGULAR((3,)), pltpu.SemaphoreType.REGULAR((2,)),
        ],
        compiler_params=pltpu.CompilerParams(collective_id=0, has_side_effects=True),
        name="subtomogram_average",
    )(orientation, wedge_index, half_set, particles[0], shell_map, first, second, back)
    return maps, fsc[0, :NSHELL]


def solution(mesh):
    both = ("px", "py")
    return jax.shard_map(
        shards,
        mesh=mesh,
        in_specs=(P(both, None, None, None, None), P(both), P(both), P(both), P(None, both, None)),
        out_specs=(P(None, None, None, both, None), P()),
        check_vma=False,
    )
```

```python
import functools
import math

import jax
import jax.numpy as jnp
import numpy as np
from jax import lax
from jax.experimental import pallas as pl
from jax.experimental.pallas import tpu as pltpu
from jax.sharding import PartitionSpec as P

RISE = (1, 3, 2, 3)
RUN = (1, 2, 1, 1)
NSHELL = 32
PLANE = 32
DEPTH = 8
LINE = 16
EXTENT = 256
BOX = 128
KZ = 128
THRESHOLDS = tuple(-(-KZ * run // rise) for rise, run in zip(RISE, RUN))
MESH = pl.DeviceIdType.MESH
f32 = jnp.float32
bf16 = jnp.bfloat16
NT = (((1,), (1,)), ((), ()))
NN = (((1,), (0,)), ((), ()))
MAPLANE = 96
TAG = 2 * 2 * DEPTH
SLAB = TAG + 1
SIGN = 16


def halves(table):
    table = jnp.asarray(table, f32)
    upper = table.astype(bf16)
    lower = (table - upper.astype(f32)).astype(bf16)
    return jnp.stack([upper, lower])


def tables():
    freq = np.arange(EXTENT)
    cell = np.arange(BOX) - BOX // 2
    scale = 1.0 / math.sqrt(EXTENT)
    unit = 2.0 * math.pi / EXTENT
    place, level = np.arange(PLANE)[:, None], np.arange(DEPTH)[None, :]
    order = (place // LINE * (LINE * DEPTH) + level * LINE + place % LINE).reshape(-1)
    angle = (order[:, None] * cell[None, :] % EXTENT) * unit
    first = np.concatenate([np.cos(angle), np.sin(angle)], 1) * scale
    angle = (cell[:, None] * freq[None, :] % EXTENT) * unit
    cosine, sine = np.cos(angle) * scale, np.sin(angle) * scale
    second = np.block([[cosine, -sine], [sine, cosine]])
    angle = (freq[:, None] * freq[None, :] % EXTENT) * unit
    back = np.concatenate([np.cos(angle), np.sin(angle)], 1) * scale
    spread = np.zeros((128, 2 * EXTENT), np.float32)
    size = np.minimum(freq, EXTENT - freq)
    for kind in range(SIGN):
        keep = size >= THRESHOLDS[kind % 4] if kind // 4 % 2 else size >= 0
        spread[kind, :EXTENT] = keep
        spread[kind, EXTENT : EXTENT + 128] = kind // 8
    spread[SIGN, EXTENT + 128 :] = 1.0
    return [np.asarray(t, np.float32) for t in (first, second, back, spread)]


def cut(value):
    upper = value.astype(bf16)
    return upper, (value - upper.astype(f32)).astype(bf16)


def dot(a, b, dims):
    return lax.dot_general(a, b, dims, preferred_element_type=f32)


def dot3(a, b, dims):
    return dot(a[0], b[0], dims) + (dot(a[0], b[1], dims) + dot(a[1], b[0], dims))


def magnitude(index):
    return jnp.minimum(index, EXTENT - index)


def pick(position, entries):
    result = jnp.full_like(position, entries[0])
    for number, entry in enumerate(entries[1:], 1):
        result = jnp.where(position == number, entry, result)
    return result


def quarter_phase(value):
    row = lax.broadcasted_iota(jnp.int32, value.shape, 0)
    return jnp.where(row // 2 % 2 == 0, -pltpu.roll(value, 6, 0), pltpu.roll(value, 2, 0))


def body(
    orient_t, wedge_t, half_t, particle, shell_t, first_t, second_t, back_t, spread_t,
    maps_ref, fsc_ref,
    orient, wedge, half, source, shell, first, second, back, spread, slab_out, slab_in,
    sum_out, sum_in, count_out, count_in, row_out, row_in, inside_ref, member_ref,
    load_sem, slab_s, slab_r, sum_s, sum_r, count_s, count_r, row_s, row_r,
    above_sem, below_sem,
):
    px, py = lax.axis_index("px"), lax.axis_index("py")
    me = px * LINE + py
    side, level = lax.div(px, DEPTH), lax.rem(px, DEPTH)
    place = side * LINE + py
    sides = [side, 1 - side]
    lines = [py] + [lax.rem(py + b, LINE) for b in range(1, LINE)]
    far_first = [8, 9, 10, 11, 7, 6, 5, 4, 12, 13, 14, 15, 3, 2, 1, 0]
    offsets = [(a, b) for b in far_first for a in (1, 0)][:-1]
    plane = [(sides[a], lines[b]) for a, b in offsets]
    slots = [offsets.index((a, (LINE - b) % LINE)) for a, b in offsets]
    levels = [level] + [lax.rem(level + c, DEPTH) for c in range(1, DEPTH)]
    column = [levels[c] for c in (4, 3, 5, 2, 6, 1, 7)]
    above = (side * DEPTH + levels[1], py)
    below = (side * DEPTH + levels[7], py)
    pairs = [
        (particle, source), (first_t, first), (orient_t, orient), (wedge_t, wedge),
        (half_t, half), (second_t, second), (spread_t, spread), (shell_t, shell), (back_t, back),
    ]
    loads = [pltpu.make_async_copy(a, b, load_sem.at[i]) for i, (a, b) in enumerate(pairs)]
    for load in loads[:5]:
        load.start()
    barrier = pltpu.get_barrier_semaphore()
    for a, b in plane:
        pl.semaphore_signal(barrier, 1, device_id=(a * DEPTH + level, b), device_id_type=MESH)
    for neighbour in (above, below):
        pl.semaphore_signal(barrier, 1, device_id=neighbour, device_id_type=MESH)

    for load in loads[5:]:
        load.start()
    for load in loads[2:5]:
        load.wait()
    turn, wedge_id, half_id = orient[0], wedge[0], half[0]
    quarter = turn % 4
    sign_x = (1 - 2 * ((quarter + 1) // 2 % 2)).astype(f32)
    sign_y = ((1 - 2 * (quarter // 2)) * (1 - 2 * (turn // 4))).astype(f32)
    swapped = turn % 2

    lane = lax.broadcasted_iota(jnp.int32, (PLANE, 128), 1)
    own_class = half_id * 8 + swapped * 4 + wedge_id
    tag = jnp.where(lane == own_class, 1.0, 0.0)
    tag = jnp.where(lane == SIGN, jnp.broadcast_to(sign_y, (PLANE, 128)), tag)
    slab_out[:, TAG, :] = tag

    row = lax.broadcasted_iota(jnp.int32, (EXTENT, 128), 0)
    kx = row // (DEPTH * LINE) * (DEPTH * LINE) + row % DEPTH * LINE + row // DEPTH % LINE
    kx_abs = magnitude(kx)
    row_limit = pick(jnp.broadcast_to(wedge_id, (EXTENT, 128)), THRESHOLDS) * (1 - swapped)
    row_mask = jnp.where(kx_abs >= row_limit, 1.0, 0.0)
    turned = jnp.broadcast_to(swapped, (BOX, BOX)) == 1
    loads[0].wait()
    loads[1].wait()
    for z in range(2):
        real, imag = source[0, z], source[1, z]
        real = jnp.where(turned, real.T, real)
        imag = jnp.where(turned, imag.T, imag)
        stacked = jnp.concatenate(
            [
                jnp.concatenate([real, imag * sign_y], 1),
                jnp.concatenate([imag * sign_x, real * (-sign_x * sign_y)], 1),
            ],
            0,
        )
        along = dot3((first[0], first[1]), cut(stacked), NN)
        if z == 0:
            along = along * jnp.concatenate([row_mask, row_mask], 1)
        for c in range(2):
            base = (2 * z + c) * DEPTH
            slab_out[:, base : base + DEPTH, :] = along[:, c * 128 : (c + 1) * 128].reshape(
                PLANE, DEPTH, 128
            )
    slab_in[PLANE - 1] = slab_out[place]
    pl.semaphore_wait(barrier, PLANE + 1)

    sent = []
    for k, (a, b) in enumerate(plane):
        sent.append(
            pltpu.make_async_remote_copy(
                slab_out.at[a * LINE + b, pl.ds(0, SLAB)], slab_in.at[slots[k], pl.ds(0, SLAB)],
                slab_s.at[k], slab_r.at[slots[k]], (a * DEPTH + level, b), MESH,
            )
        )
    for copy in sent:
        copy.start()
    for step in range(3):
        pl.semaphore_signal(above_sem.at[step], 1, device_id=above, device_id_type=MESH)
        if step < 2:
            pl.semaphore_signal(below_sem.at[step], 1, device_id=below, device_id_type=MESH)
            pl.semaphore_wait(below_sem.at[step], 1)
        pl.semaphore_wait(above_sem.at[step], 1)
    kind = lax.broadcasted_iota(jnp.int32, (128, EXTENT), 0)
    ky_wide = magnitude(lax.broadcasted_iota(jnp.int32, (128, EXTENT), 1))
    reach = jnp.where(kind // 4 % 2 == 1, ky_wide, magnitude(me))
    inside_ref[...] = jnp.where(reach >= pick(kind % 4, THRESHOLDS), 1.0, 0.0).astype(bf16)
    for load in loads[5:]:
        load.wait()
    number = kind % NSHELL
    for z in range(2):
        member_ref[z] = jnp.where(number == shell[z], 1.0, 0.0).astype(bf16)

    second_pair = (second[0], second[1])
    spread_map = spread[...]
    totals = [[jnp.zeros((DEPTH, 2 * EXTENT), f32) for z in range(2)] for h in range(2)]
    counts = jnp.zeros((1, 128), f32)
    group = 8
    arrivals = {slots[k]: copy for k, copy in enumerate(sent)}
    for start in range(PLANE - group, -1, -group):
        for k in range(start, min(start + group, PLANE - 1)):
            arrivals[k].wait_recv()
        tags = slab_in[start : start + group, TAG, :]
        counts = counts + jnp.sum(tags, axis=0, keepdims=True)
        vectors = dot(tags.astype(bf16), spread_map, NN)
        blocks = []
        for z in range(2):
            real = slab_in[start : start + group, 2 * z * DEPTH : (2 * z + 1) * DEPTH, :]
            imag = slab_in[start : start + group, (2 * z + 1) * DEPTH : (2 * z + 2) * DEPTH, :]
            blocks.append(jnp.concatenate([real, imag], 2).reshape(group * DEPTH, EXTENT))
        waves = dot3(cut(jnp.concatenate(blocks, 0)), second_pair, NN)
        for g in range(group):
            vector = vectors[g : g + 1]
            keep = vector[:, :EXTENT]
            lane_half = jnp.concatenate([vector[:, EXTENT : EXTENT + 128]] * 4, 1)
            lane_sign = jnp.concatenate([vector[:, EXTENT + 128 :]] * 2, 1)
            factors = (
                jnp.concatenate([keep, keep * lane_sign], 1),
                jnp.concatenate([jnp.ones_like(keep), lane_sign], 1),
            )
            for z in range(2):
                base = (z * group + g) * DEPTH
                value = waves[base : base + DEPTH] * factors[z]
                upper = value * lane_half
                totals[1][z] = totals[1][z] + upper
                totals[0][z] = totals[0][z] + (value - upper)
    for h in range(2):
        for c in range(2):
            for z in range(2):
                sum_out[:, h * 4 + c * 2 + z, :] = totals[h][z][:, c * EXTENT : (c + 1) * EXTENT]
    count_out[...] = counts
    count_in[level] = counts
    sum_in[level] = sum_out[level]

    summed = []
    for k, other in enumerate(column):
        to = (side * DEPTH + other, py)
        summed.append(
            pltpu.make_async_remote_copy(
                count_out, count_in.at[level], count_s.at[k], count_r.at[k], to, MESH
            )
        )
        summed.append(
            pltpu.make_async_remote_copy(
                sum_out.at[other], sum_in.at[level], sum_s.at[k], sum_r.at[k], to, MESH
            )
        )
    for copy in summed:
        copy.start()
    comp = lax.broadcasted_iota(jnp.int32, (8, 128), 0)
    lane = lax.broadcasted_iota(jnp.int32, (8, 128), 1)
    inside = inside_ref[...]
    members = [member_ref[0], member_ref[1]]
    for copy in summed:
        copy.wait_recv()
    total = sum_in[0]
    count = count_in[0]
    for k in range(1, DEPTH):
        total = total + sum_in[k]
        count = count + count_in[k]
    by_half = jnp.where(lane // 8 == comp // 4, count, 0.0)
    masked_count = dot(by_half.astype(bf16), inside, NN)
    full_count = jnp.sum(by_half, axis=1, keepdims=True)
    wide_comp = lax.broadcasted_iota(jnp.int32, (8, EXTENT), 0)
    cover = jnp.where(wide_comp % 2 == 0, masked_count, full_count)
    average = total / jnp.maximum(cover, 1.0)

    powers = jnp.concatenate([average * average, average * pltpu.roll(average, 4, 0)], 0)
    powers = cut(powers)
    p_row = lax.broadcasted_iota(jnp.int32, (16, 128), 0)
    p_lane = lax.broadcasted_iota(jnp.int32, (16, 128), 1)
    wanted = jnp.where(p_row < 8, 1 + p_row // 4, jnp.where(p_row < 12, 0, 4))
    shells = jnp.zeros((1, 128), f32)
    for z in range(2):
        part = dot(powers[0], members[z], NT) + dot(powers[1], members[z], NT)
        part = jnp.where((p_row % 2 == z) & (p_lane // NSHELL == wanted), part, 0.0)
        shells = shells + jnp.sum(part, axis=0, keepdims=True)

    back_pair = (back[0], back[1])
    pair = jnp.concatenate([average, quarter_phase(average)], 1)
    padded = jnp.concatenate(
        [
            jnp.zeros((MAPLANE, 2 * EXTENT), f32),
            pair,
            jnp.zeros((128 - MAPLANE - 8, 2 * EXTENT), f32),
        ],
        0,
    )
    middle = dot3(back_pair, cut(padded), NT)
    row_out[...] = middle + shells
    row_in[pl.ds(me, 1)] = row_out[pl.ds(me, 1)]

    def send_row(a, c, b):
        to = (a * DEPTH + c, b)
        other = to[0] * LINE + b
        pltpu.make_async_remote_copy(
            row_out.at[pl.ds(other, 1)], row_in.at[pl.ds(me, 1)], row_s, row_r, to, MESH
        ).start()

    @pl.loop(0, DEPTH - 1)
    def _(step):
        away = lax.div(step + 1, 2)
        shift = away * (1 - 2 * lax.rem(step, 2))
        other = lax.rem(level + 12 + shift, DEPTH)
        for a, b in plane + [(side, py)]:
            send_row(a, other, b)

    for a, b in plane:
        send_row(a, level, b)

    whole = row_in.at[pl.ds(0, EXTENT - 1)]
    pltpu.make_async_copy(whole, whole, row_r).wait()
    rows = row_in[...]
    sums = jnp.sum(rows, axis=0, keepdims=True)
    values = rows.T[MAPLANE : MAPLANE + 8]
    pair = jnp.concatenate([values, quarter_phase(values)], 1)
    final = dot3(cut(pair), back_pair, NT)
    maps_ref[...] = final
    sums = jnp.broadcast_to(sums, (8, 128))
    first_power = pltpu.roll(sums, 128 - NSHELL, 1)
    second_power = pltpu.roll(sums, 128 - 2 * NSHELL, 1)
    fsc_ref[...] = sums / (jnp.sqrt(first_power * second_power) + 1e-06)

    for copy in sent + summed:
        copy.wait_send()
    pltpu.make_async_copy(whole, whole, row_s).wait()


def finish(final, shells, maps_ref, fsc_ref):
    for h in range(2):
        for c in range(2):
            for z in range(2):
                n = h * 4 + c * 2 + z
                maps_ref[h, c, z] = final[n : n + 1]
    fsc_ref[...] = shells[0, :NSHELL]


def shards(particles, orientation, wedge_index, half_set, shell_map):
    first, second, back, spread = tables()
    first, second, back = (halves(t) for t in (first, second, back))
    spread = jnp.asarray(spread, bf16)
    vmem = pl.BlockSpec(memory_space=pltpu.VMEM)
    hbm = pl.BlockSpec(memory_space=pltpu.HBM)
    dma = pltpu.SemaphoreType.DMA
    final, shells = pl.pallas_call(
        body,
        out_shape=(
            pltpu.VMEM((8, EXTENT), f32),
            pltpu.VMEM((8, 128), f32),
        ),
        in_specs=[hbm] * 9,
        out_specs=(vmem, vmem),
        scratch_shapes=[
            pltpu.SMEM((1,), jnp.int32), pltpu.SMEM((1,), jnp.int32), pltpu.SMEM((1,), jnp.int32),
            pltpu.VMEM((2, 2, BOX, BOX), f32),
            pltpu.VMEM((2, 1, EXTENT), jnp.int32),
            pltpu.VMEM((2, EXTENT, EXTENT), bf16),
            pltpu.VMEM((2, EXTENT, 2 * EXTENT), bf16),
            pltpu.VMEM((2, EXTENT, 2 * EXTENT), bf16),
            pltpu.VMEM((128, 2 * EXTENT), bf16),
            pltpu.VMEM((PLANE, SLAB + 7, 128), f32),
            pltpu.VMEM((PLANE, SLAB + 7, 128), f32),
            pltpu.VMEM((DEPTH, 8, EXTENT), f32),
            pltpu.VMEM((DEPTH, 8, EXTENT), f32),
            pltpu.VMEM((1, 128), f32),
            pltpu.VMEM((DEPTH, 1, 128), f32),
            pltpu.VMEM((EXTENT, 128), f32),
            pltpu.VMEM((EXTENT, 128), f32),
            pltpu.VMEM((128, EXTENT), bf16),
            pltpu.VMEM((2, 128, EXTENT), bf16),
            dma((9,)),
            dma((PLANE,)), dma((PLANE,)),
            dma((DEPTH,)), dma((DEPTH,)), dma((DEPTH,)), dma((DEPTH,)),
            dma, dma,
            pltpu.SemaphoreType.REGULAR((3,)), pltpu.SemaphoreType.REGULAR((2,)),
        ],
        compiler_params=pltpu.CompilerParams(collective_id=0, has_side_effects=True),
        name="subtomogram_average",
    )(
        orientation, wedge_index, half_set, particles[0], shell_map, first, second, back, spread
    )
    final = pltpu.with_memory_space_constraint(final, pltpu.VMEM)
    shells = pltpu.with_memory_space_constraint(shells, pltpu.VMEM)
    return pl.pallas_call(
        finish,
        out_shape=(
            jax.ShapeDtypeStruct((2, 2, 2, 1, EXTENT), f32),
            jax.ShapeDtypeStruct((NSHELL,), f32),
        ),
        in_specs=[vmem, vmem],
        out_specs=(vmem, vmem),
        name="hand_out",
    )(final, shells)


def solution(mesh):
    both = ("px", "py")
    return jax.shard_map(
        shards,
        mesh=mesh,
        in_specs=(P(both, None, None, None, None), P(both), P(both), P(both), P(None, both, None)),
        out_specs=(P(None, None, None, both, None), P()),
        check_vma=False,
    )
```

```python
import functools
import math

import jax
import jax.numpy as jnp
import numpy as np
from jax import lax
from jax.experimental import pallas as pl
from jax.experimental.pallas import tpu as pltpu
from jax.sharding import PartitionSpec as P

RISE = (1, 3, 2, 3)
RUN = (1, 2, 1, 1)
NSHELL = 32
PLANE = 32
DEPTH = 8
LINE = 16
EXTENT = 256
BOX = 128
KZ = 128
THRESHOLDS = tuple(-(-KZ * run // rise) for rise, run in zip(RISE, RUN))
MESH = pl.DeviceIdType.MESH
f32 = jnp.float32
bf16 = jnp.bfloat16
NT = (((1,), (1,)), ((), ()))
NN = (((1,), (0,)), ((), ()))
MAPLANE = 96
GROUPS = (8, 8, 8, 8)
SUMS = 17
TAG = 2 * 2 * DEPTH
SLAB = TAG + 1
SIGN = 16


def halves(table):
    table = jnp.asarray(table, f32)
    upper = table.astype(bf16)
    lower = (table - upper.astype(f32)).astype(bf16)
    return jnp.stack([upper, lower])


def tables():
    freq = np.arange(EXTENT)
    cell = np.arange(BOX) - BOX // 2
    scale = 1.0 / math.sqrt(EXTENT)
    unit = 2.0 * math.pi / EXTENT
    place, level = np.arange(PLANE)[:, None], np.arange(DEPTH)[None, :]
    order = (place // LINE * (LINE * DEPTH) + level * LINE + place % LINE).reshape(-1)
    angle = (order[:, None] * cell[None, :] % EXTENT) * unit
    first = np.concatenate([np.cos(angle), np.sin(angle)], 1) * scale
    angle = (cell[:, None] * freq[None, :] % EXTENT) * unit
    cosine, sine = np.cos(angle) * scale, np.sin(angle) * scale
    second = np.block([[cosine, -sine], [sine, cosine]])
    angle = (freq[:, None] * freq[None, :] % EXTENT) * unit
    back = np.concatenate([np.cos(angle), np.sin(angle)], 1) * scale
    spread = np.zeros((128, 2 * EXTENT), np.float32)
    size = np.minimum(freq, EXTENT - freq)
    for kind in range(SIGN):
        keep = size >= THRESHOLDS[kind % 4] if kind // 4 % 2 else size >= 0
        spread[kind, :EXTENT] = keep
        spread[kind, EXTENT : EXTENT + 128] = kind // 8
    spread[SIGN, EXTENT + 128 :] = 1.0
    return [np.asarray(t, np.float32) for t in (first, second, back, spread)]


def cut(value):
    upper = value.astype(bf16)
    return upper, (value - upper.astype(f32)).astype(bf16)


def dot(a, b, dims):
    return lax.dot_general(a, b, dims, preferred_element_type=f32)


def dot3(a, b, dims):
    return dot(a[0], b[0], dims) + (dot(a[0], b[1], dims) + dot(a[1], b[0], dims))


def magnitude(index):
    return jnp.minimum(index, EXTENT - index)


def pick(position, entries):
    result = jnp.full_like(position, entries[0])
    for number, entry in enumerate(entries[1:], 1):
        result = jnp.where(position == number, entry, result)
    return result


def quarter_phase(value):
    row = lax.broadcasted_iota(jnp.int32, value.shape, 0)
    return jnp.where(row // 2 % 2 == 0, -pltpu.roll(value, 6, 0), pltpu.roll(value, 2, 0))


def body(
    orient_t, wedge_t, half_t, particle, shell_t, first_t, second_t, back_t, spread_t,
    maps_ref, fsc_ref,
    orient, wedge, half, source, shell, first, second, back, spread, slab_out, slab_in,
    sum_out, sum_in, row_out, row_in, inside_ref, member_ref,
    load_sem, slab_s, slab_r, sum_s, sum_r, row_s, row_r,
    above_sem, below_sem,
):
    px, py = lax.axis_index("px"), lax.axis_index("py")
    me = px * LINE + py
    side, level = lax.div(px, DEPTH), lax.rem(px, DEPTH)
    place = side * LINE + py
    y = lax.div(py, 4)
    ys = [y] + [lax.rem(y + b, 4) for b in range(1, 4)]
    near_bit, core = lax.rem(lax.div(py, 2), 2), lax.rem(py, 2)
    low = [near_bit * 2 + core, near_bit * 2 + 1 - core]
    low += [2 - near_bit * 2 + core, 3 - near_bit * 2 - core]
    sides = [side, 1 - side]
    offsets = [(1, 2, 1), (1, 2, 0), (0, 2, 3), (1, 1, 1), (1, 2, 3), (1, 3, 1), (0, 2, 2), (1, 1, 0), (1, 2, 2), (1, 3, 0), (0, 1, 3), (0, 2, 1), (0, 3, 3), (1, 0, 1), (1, 1, 3), (1, 3, 3), (0, 1, 2), (0, 2, 0), (0, 3, 2), (1, 0, 0), (1, 1, 2), (1, 3, 2), (0, 0, 3), (0, 1, 1), (0, 3, 1), (1, 0, 3), (0, 0, 2), (0, 1, 0), (0, 3, 0), (1, 0, 2), (0, 0, 1)]
    bunch = [n for n, size in enumerate(GROUPS) for _ in range(size)]
    plane = [(sides[a], ys[b] * 4 + low[c]) for a, b, c in offsets]
    slots = [offsets.index((a, (4 - b) % 4, c)) for a, b, c in offsets]
    levels = [level] + [lax.rem(level + c, DEPTH) for c in range(1, DEPTH)]
    column = [levels[c] for c in (4, 3, 5, 2, 6, 1, 7)]
    above = (side * DEPTH + levels[1], py)
    below = (side * DEPTH + levels[7], py)
    pairs = [
        (particle, source), (first_t, first), (orient_t, orient), (wedge_t, wedge),
        (half_t, half), (second_t, second), (spread_t, spread), (shell_t, shell), (back_t, back),
    ]
    loads = [pltpu.make_async_copy(a, b, load_sem.at[i]) for i, (a, b) in enumerate(pairs)]
    barrier = pltpu.get_barrier_semaphore()
    for a, b in plane:
        pl.semaphore_signal(barrier, 1, device_id=(a * DEPTH + level, b), device_id_type=MESH)
    for neighbour in (above, below):
        pl.semaphore_signal(barrier, 1, device_id=neighbour, device_id_type=MESH)

    for load in loads:
        load.start()
    for load in loads[2:5]:
        load.wait()
    turn, wedge_id, half_id = orient[0], wedge[0], half[0]
    quarter = turn % 4
    sign_x = (1 - 2 * ((quarter + 1) // 2 % 2)).astype(f32)
    sign_y = ((1 - 2 * (quarter // 2)) * (1 - 2 * (turn // 4))).astype(f32)
    swapped = turn % 2

    lane = lax.broadcasted_iota(jnp.int32, (PLANE, 128), 1)
    own_class = half_id * 8 + swapped * 4 + wedge_id
    tag = jnp.where(lane == own_class, 1.0, 0.0)
    tag = jnp.where(lane == SIGN, jnp.broadcast_to(sign_y, (PLANE, 128)), tag)
    slab_out[:, TAG, :] = tag

    row = lax.broadcasted_iota(jnp.int32, (EXTENT, 128), 0)
    kx = row // (DEPTH * LINE) * (DEPTH * LINE) + row % DEPTH * LINE + row // DEPTH % LINE
    kx_abs = magnitude(kx)
    row_limit = pick(jnp.broadcast_to(wedge_id, (EXTENT, 128)), THRESHOLDS) * (1 - swapped)
    row_mask = jnp.where(kx_abs >= row_limit, 1.0, 0.0)
    turned = jnp.broadcast_to(swapped, (BOX, BOX)) == 1
    loads[0].wait()
    loads[1].wait()
    for z in range(2):
        real, imag = source[0, z], source[1, z]
        real = jnp.where(turned, real.T, real)
        imag = jnp.where(turned, imag.T, imag)
        stacked = jnp.concatenate(
            [
                jnp.concatenate([real, imag * sign_y], 1),
                jnp.concatenate([imag * sign_x, real * (-sign_x * sign_y)], 1),
            ],
            0,
        )
        along = dot3((first[0], first[1]), cut(stacked), NN)
        if z == 0:
            along = along * jnp.concatenate([row_mask, row_mask], 1)
        for c in range(2):
            base = (2 * z + c) * DEPTH
            slab_out[:, base : base + DEPTH, :] = along[:, c * 128 : (c + 1) * 128].reshape(
                PLANE, DEPTH, 128
            )
    slab_in[PLANE - 1] = slab_out[place]
    pl.semaphore_wait(barrier, PLANE + 1)

    for k, (a, b) in enumerate(plane):
        pltpu.make_async_remote_copy(
            slab_out.at[a * LINE + b, pl.ds(0, SLAB)], slab_in.at[slots[k], pl.ds(0, SLAB)],
            slab_s, slab_r.at[bunch[slots[k]]], (a * DEPTH + level, b), MESH,
        ).start()
    for step in range(3):
        pl.semaphore_signal(above_sem.at[step], 1, device_id=above, device_id_type=MESH)
        if step < 2:
            pl.semaphore_signal(below_sem.at[step], 1, device_id=below, device_id_type=MESH)
            pl.semaphore_wait(below_sem.at[step], 1)
        pl.semaphore_wait(above_sem.at[step], 1)
    kind = lax.broadcasted_iota(jnp.int32, (128, EXTENT), 0)
    ky_wide = magnitude(lax.broadcasted_iota(jnp.int32, (128, EXTENT), 1))
    reach = jnp.where(kind // 4 % 2 == 1, ky_wide, magnitude(me))
    inside_ref[...] = jnp.where(reach >= pick(kind % 4, THRESHOLDS), 1.0, 0.0).astype(bf16)
    for load in loads[5:]:
        load.wait()
    number = kind % NSHELL
    for z in range(2):
        member_ref[z] = jnp.where(number == shell[z], 1.0, 0.0).astype(bf16)

    second_pair = (second[0], second[1])
    spread_map = spread[...]
    totals = [[jnp.zeros((DEPTH, 2 * EXTENT), f32) for z in range(2)] for h in range(2)]
    counts = jnp.zeros((1, 128), f32)
    for turn_in, group in enumerate(GROUPS):
        start = sum(GROUPS[:turn_in])
        landed = slab_in.at[pl.ds(start, min(group, PLANE - 1 - start)), pl.ds(0, SLAB)]
        pltpu.make_async_copy(landed, landed, slab_r.at[turn_in]).wait()
        tags = slab_in[start : start + group, TAG, :]
        counts = counts + jnp.sum(tags, axis=0, keepdims=True)
        vectors = dot(tags.astype(bf16), spread_map, NN)
        blocks = []
        for z in range(2):
            real = slab_in[start : start + group, 2 * z * DEPTH : (2 * z + 1) * DEPTH, :]
            imag = slab_in[start : start + group, (2 * z + 1) * DEPTH : (2 * z + 2) * DEPTH, :]
            blocks.append(jnp.concatenate([real, imag], 2).reshape(group * DEPTH, EXTENT))
        waves = dot3(cut(jnp.concatenate(blocks, 0)), second_pair, NN)
        for g in range(group):
            vector = vectors[g : g + 1]
            keep = vector[:, :EXTENT]
            lane_half = jnp.concatenate([vector[:, EXTENT : EXTENT + 128]] * 4, 1)
            lane_sign = jnp.concatenate([vector[:, EXTENT + 128 :]] * 2, 1)
            factors = (
                jnp.concatenate([keep, keep * lane_sign], 1),
                jnp.concatenate([jnp.ones_like(keep), lane_sign], 1),
            )
            for z in range(2):
                base = (z * group + g) * DEPTH
                value = waves[base : base + DEPTH] * factors[z]
                upper = value * lane_half
                totals[1][z] = totals[1][z] + upper
                totals[0][z] = totals[0][z] + (value - upper)
    for h in range(2):
        for c in range(2):
            for z in range(2):
                for q in range(2):
                    base = c * EXTENT + q * 128
                    sum_out[:, q * 8 + h * 4 + c * 2 + z, :] = totals[h][z][:, base : base + 128]
    sum_out[:, SUMS - 1, :] = jnp.broadcast_to(counts, (DEPTH, 128))
    sum_in[level] = sum_out[level]

    for other in column:
        pltpu.make_async_remote_copy(
            sum_out.at[other, pl.ds(0, SUMS)], sum_in.at[level, pl.ds(0, SUMS)],
            sum_s, sum_r, (side * DEPTH + other, py), MESH,
        ).start()
    comp = lax.broadcasted_iota(jnp.int32, (8, 128), 0)
    lane = lax.broadcasted_iota(jnp.int32, (8, 128), 1)
    inside = inside_ref[...]
    members = [member_ref[0], member_ref[1]]
    landed = sum_in.at[pl.ds(0, DEPTH - 1), pl.ds(0, SUMS)]
    pltpu.make_async_copy(landed, landed, sum_r).wait()
    total = sum_in[0, :SUMS]
    for k in range(1, DEPTH):
        total = total + sum_in[k, :SUMS]
    count = total[SUMS - 1 :]
    total = jnp.concatenate([total[:8], total[8:16]], 1)
    by_half = jnp.where(lane // 8 == comp // 4, count, 0.0)
    masked_count = dot(by_half.astype(bf16), inside, NN)
    full_count = jnp.sum(by_half, axis=1, keepdims=True)
    wide_comp = lax.broadcasted_iota(jnp.int32, (8, EXTENT), 0)
    cover = jnp.where(wide_comp % 2 == 0, masked_count, full_count)
    average = total / jnp.maximum(cover, 1.0)

    powers = jnp.concatenate([average * average, average * pltpu.roll(average, 4, 0)], 0)
    powers = cut(powers)
    p_row = lax.broadcasted_iota(jnp.int32, (16, 128), 0)
    p_lane = lax.broadcasted_iota(jnp.int32, (16, 128), 1)
    wanted = jnp.where(p_row < 8, 1 + p_row // 4, jnp.where(p_row < 12, 0, 4))
    shells = jnp.zeros((1, 128), f32)
    for z in range(2):
        part = dot(powers[0], members[z], NT) + dot(powers[1], members[z], NT)
        part = jnp.where((p_row % 2 == z) & (p_lane // NSHELL == wanted), part, 0.0)
        shells = shells + jnp.sum(part, axis=0, keepdims=True)

    back_pair = (back[0], back[1])
    pair = jnp.concatenate([average, quarter_phase(average)], 1)
    padded = jnp.concatenate(
        [
            jnp.zeros((MAPLANE, 2 * EXTENT), f32),
            pair,
            jnp.zeros((128 - MAPLANE - 8, 2 * EXTENT), f32),
        ],
        0,
    )
    middle = dot3(back_pair, cut(padded), NT)
    row_out[...] = middle + shells
    row_in[pl.ds(me, 1)] = row_out[pl.ds(me, 1)]

    def send_row(a, c, b):
        to = (a * DEPTH + c, b)
        other = to[0] * LINE + b
        pltpu.make_async_remote_copy(
            row_out.at[pl.ds(other, 1)], row_in.at[pl.ds(me, 1)], row_s, row_r, to, MESH
        ).start()

    @pl.loop(0, DEPTH - 1)
    def _(step):
        away = lax.div(step + 1, 2)
        shift = away * (1 - 2 * lax.rem(step, 2))
        other = lax.rem(level + 12 + shift, DEPTH)
        for a, b in plane + [(side, py)]:
            send_row(a, other, b)

    for a, b in plane:
        send_row(a, level, b)

    whole = row_in.at[pl.ds(0, EXTENT - 1)]
    pltpu.make_async_copy(whole, whole, row_r).wait()
    rows = row_in[...]
    sums = jnp.sum(rows, axis=0, keepdims=True)
    values = rows.T[MAPLANE : MAPLANE + 8]
    pair = jnp.concatenate([values, quarter_phase(values)], 1)
    final = dot3(cut(pair), back_pair, NT)
    maps_ref[...] = final
    sums = jnp.broadcast_to(sums, (8, 128))
    first_power = pltpu.roll(sums, 128 - NSHELL, 1)
    second_power = pltpu.roll(sums, 128 - 2 * NSHELL, 1)
    fsc_ref[...] = sums / (jnp.sqrt(first_power * second_power) + 1e-06)

    gone = slab_out.at[pl.ds(0, PLANE - 1), pl.ds(0, SLAB)]
    pltpu.make_async_copy(gone, gone, slab_s).wait()
    pltpu.make_async_copy(landed, landed, sum_s).wait()
    pltpu.make_async_copy(whole, whole, row_s).wait()


def finish(final, shells, maps_ref, fsc_ref):
    for h in range(2):
        for c in range(2):
            for z in range(2):
                n = h * 4 + c * 2 + z
                maps_ref[h, c, z] = final[n : n + 1]
    fsc_ref[...] = shells[0, :NSHELL]


def shards(particles, orientation, wedge_index, half_set, shell_map):
    first, second, back, spread = tables()
    first, second, back = (halves(t) for t in (first, second, back))
    spread = jnp.asarray(spread, bf16)
    vmem = pl.BlockSpec(memory_space=pltpu.VMEM)
    hbm = pl.BlockSpec(memory_space=pltpu.HBM)
    dma = pltpu.SemaphoreType.DMA
    final, shells = pl.pallas_call(
        body,
        out_shape=(
            pltpu.VMEM((8, EXTENT), f32),
            pltpu.VMEM((8, 128), f32),
        ),
        in_specs=[hbm] * 9,
        out_specs=(vmem, vmem),
        scratch_shapes=[
            pltpu.SMEM((1,), jnp.int32), pltpu.SMEM((1,), jnp.int32), pltpu.SMEM((1,), jnp.int32),
            pltpu.VMEM((2, 2, BOX, BOX), f32),
            pltpu.VMEM((2, 1, EXTENT), jnp.int32),
            pltpu.VMEM((2, EXTENT, EXTENT), bf16),
            pltpu.VMEM((2, EXTENT, 2 * EXTENT), bf16),
            pltpu.VMEM((2, EXTENT, 2 * EXTENT), bf16),
            pltpu.VMEM((128, 2 * EXTENT), bf16),
            pltpu.VMEM((PLANE, SLAB + 7, 128), f32),
            pltpu.VMEM((PLANE, SLAB + 7, 128), f32),
            pltpu.VMEM((DEPTH, SUMS + 7, 128), f32),
            pltpu.VMEM((DEPTH, SUMS + 7, 128), f32),
            pltpu.VMEM((EXTENT, 128), f32),
            pltpu.VMEM((EXTENT, 128), f32),
            pltpu.VMEM((128, EXTENT), bf16),
            pltpu.VMEM((2, 128, EXTENT), bf16),
            dma((9,)),
            dma, dma((len(GROUPS),)), dma, dma, dma, dma,
            pltpu.SemaphoreType.REGULAR((3,)), pltpu.SemaphoreType.REGULAR((2,)),
        ],
        compiler_params=pltpu.CompilerParams(collective_id=0, has_side_effects=True),
        name="subtomogram_average",
    )(
        orientation, wedge_index, half_set, particles[0], shell_map, first, second, back, spread
    )
    final = pltpu.with_memory_space_constraint(final, pltpu.VMEM)
    shells = pltpu.with_memory_space_constraint(shells, pltpu.VMEM)
    return pl.pallas_call(
        finish,
        out_shape=(
            jax.ShapeDtypeStruct((2, 2, 2, 1, EXTENT), f32),
            jax.ShapeDtypeStruct((NSHELL,), f32),
        ),
        in_specs=[vmem, vmem],
        out_specs=(vmem, vmem),
        name="hand_out",
    )(final, shells)


def solution(mesh):
    both = ("px", "py")
    return jax.shard_map(
        shards,
        mesh=mesh,
        in_specs=(P(both, None, None, None, None), P(both), P(both), P(both), P(None, both, None)),
        out_specs=(P(None, None, None, both, None), P()),
        check_vma=False,
    )
```

```python
import functools
import math

import jax
import jax.numpy as jnp
import numpy as np
from jax import lax
from jax.experimental import pallas as pl
from jax.experimental.pallas import tpu as pltpu
from jax.sharding import PartitionSpec as P

RISE = (1, 3, 2, 3)
RUN = (1, 2, 1, 1)
NSHELL = 32
PLANE = 32
DEPTH = 8
LINE = 16
EXTENT = 256
BOX = 128
KZ = 128
THRESHOLDS = tuple(-(-KZ * run // rise) for rise, run in zip(RISE, RUN))
MESH = pl.DeviceIdType.MESH
f32 = jnp.float32
bf16 = jnp.bfloat16
NT = (((1,), (1,)), ((), ()))
NN = (((1,), (0,)), ((), ()))
MAPLANE = 96
GROUPS = (8, 8, 8, 8)
SUMS = 17
TAG = 2 * 2 * DEPTH
SLAB = TAG + 1
SIGN = 16


def halves(table):
    table = jnp.asarray(table, f32)
    upper = table.astype(bf16)
    lower = (table - upper.astype(f32)).astype(bf16)
    return jnp.stack([upper, lower])


def tables():
    freq = np.arange(EXTENT)
    cell = np.arange(BOX) - BOX // 2
    scale = 1.0 / math.sqrt(EXTENT)
    unit = 2.0 * math.pi / EXTENT
    place, level = np.arange(PLANE)[:, None], np.arange(DEPTH)[None, :]
    order = (place // LINE * (LINE * DEPTH) + level * LINE + place % LINE).reshape(-1)
    angle = (order[:, None] * cell[None, :] % EXTENT) * unit
    first = np.concatenate([np.cos(angle), np.sin(angle)], 1) * scale
    angle = (cell[:, None] * freq[None, :] % EXTENT) * unit
    cosine, sine = np.cos(angle) * scale, np.sin(angle) * scale
    second = np.block([[cosine, -sine], [sine, cosine]])
    angle = (freq[:, None] * freq[None, :] % EXTENT) * unit
    back = np.concatenate([np.cos(angle), np.sin(angle)], 0) * scale
    spread = np.zeros((128, 2 * EXTENT), np.float32)
    size = np.minimum(freq, EXTENT - freq)
    for kind in range(SIGN):
        keep = size >= THRESHOLDS[kind % 4] if kind // 4 % 2 else size >= 0
        spread[kind, :EXTENT] = keep
        spread[kind, EXTENT : EXTENT + 128] = kind // 8
    spread[SIGN, EXTENT + 128 :] = 1.0
    return [np.asarray(t, np.float32) for t in (first, second, back, spread)]


def cut(value):
    upper = value.astype(bf16)
    return upper, (value - upper.astype(f32)).astype(bf16)


def dot(a, b, dims):
    return lax.dot_general(a, b, dims, preferred_element_type=f32)


def dot3(a, b, dims):
    return dot(a[0], b[0], dims) + (dot(a[0], b[1], dims) + dot(a[1], b[0], dims))


def dot3_few(a, b):
    rows = a.shape[0]
    upper, lower = cut(a)
    both = dot(jnp.concatenate([upper, lower], 0), b[0], NN)
    return both[:rows] + (both[rows:] + dot(upper, b[1], NN))


def magnitude(index):
    return jnp.minimum(index, EXTENT - index)


def pick(position, entries):
    result = jnp.full_like(position, entries[0])
    for number, entry in enumerate(entries[1:], 1):
        result = jnp.where(position == number, entry, result)
    return result


def quarter_phase(value):
    row = lax.broadcasted_iota(jnp.int32, value.shape, 0)
    return jnp.where(row // 2 % 2 == 0, -pltpu.roll(value, 6, 0), pltpu.roll(value, 2, 0))


def body(
    orient_t, wedge_t, half_t, particle, shell_t, first_t, second_t, back_t, spread_t,
    maps_ref, fsc_ref,
    orient, wedge, half, source, shell, first, second, back, spread, slab_out, slab_in,
    sum_out, sum_in, row_out, row_in, inside_ref, member_ref,
    load_sem, slab_s, slab_r, sum_s, sum_r, row_s, row_r,
    above_sem, below_sem,
):
    px, py = lax.axis_index("px"), lax.axis_index("py")
    me = px * LINE + py
    side, level = lax.div(px, DEPTH), lax.rem(px, DEPTH)
    place = side * LINE + py
    y = lax.div(py, 4)
    ys = [y] + [lax.rem(y + b, 4) for b in range(1, 4)]
    near_bit, core = lax.rem(lax.div(py, 2), 2), lax.rem(py, 2)
    low = [near_bit * 2 + core, near_bit * 2 + 1 - core]
    low += [2 - near_bit * 2 + core, 3 - near_bit * 2 - core]
    sides = [side, 1 - side]
    offsets = [(1, 2, 1), (1, 2, 0), (0, 2, 3), (1, 1, 1), (1, 2, 3), (1, 3, 1), (0, 2, 2), (1, 1, 0), (1, 2, 2), (1, 3, 0), (0, 1, 3), (0, 2, 1), (0, 3, 3), (1, 0, 1), (1, 1, 3), (1, 3, 3), (0, 1, 2), (0, 2, 0), (0, 3, 2), (1, 0, 0), (1, 1, 2), (1, 3, 2), (0, 0, 3), (0, 1, 1), (0, 3, 1), (1, 0, 3), (0, 0, 2), (0, 1, 0), (0, 3, 0), (1, 0, 2), (0, 0, 1)]
    bunch = [n for n, size in enumerate(GROUPS) for _ in range(size)]
    plane = [(sides[a], ys[b] * 4 + low[c]) for a, b, c in offsets]
    slots = [offsets.index((a, (4 - b) % 4, c)) for a, b, c in offsets]
    levels = [level] + [lax.rem(level + c, DEPTH) for c in range(1, DEPTH)]
    column = [levels[c] for c in (4, 3, 5, 2, 6, 1, 7)]
    above = (side * DEPTH + levels[1], py)
    below = (side * DEPTH + levels[7], py)
    pairs = [
        (particle, source), (first_t, first), (orient_t, orient), (wedge_t, wedge),
        (half_t, half), (second_t, second), (spread_t, spread), (shell_t, shell), (back_t, back),
    ]
    loads = [pltpu.make_async_copy(a, b, load_sem.at[i]) for i, (a, b) in enumerate(pairs)]
    barrier = pltpu.get_barrier_semaphore()
    for a, b in plane:
        pl.semaphore_signal(barrier, 1, device_id=(a * DEPTH + level, b), device_id_type=MESH)
    for neighbour in (above, below):
        pl.semaphore_signal(barrier, 1, device_id=neighbour, device_id_type=MESH)

    for load in loads:
        load.start()
    for load in loads[2:5]:
        load.wait()
    turn, wedge_id, half_id = orient[0], wedge[0], half[0]
    quarter = turn % 4
    sign_x = (1 - 2 * ((quarter + 1) // 2 % 2)).astype(f32)
    sign_y = ((1 - 2 * (quarter // 2)) * (1 - 2 * (turn // 4))).astype(f32)
    swapped = turn % 2

    lane = lax.broadcasted_iota(jnp.int32, (PLANE, 128), 1)
    own_class = half_id * 8 + swapped * 4 + wedge_id
    tag = jnp.where(lane == own_class, 1.0, 0.0)
    tag = jnp.where(lane == SIGN, jnp.broadcast_to(sign_y, (PLANE, 128)), tag)
    slab_out[:, TAG, :] = tag

    row = lax.broadcasted_iota(jnp.int32, (EXTENT, 128), 0)
    kx = row // (DEPTH * LINE) * (DEPTH * LINE) + row % DEPTH * LINE + row // DEPTH % LINE
    kx_abs = magnitude(kx)
    row_limit = pick(jnp.broadcast_to(wedge_id, (EXTENT, 128)), THRESHOLDS) * (1 - swapped)
    row_mask = jnp.where(kx_abs >= row_limit, 1.0, 0.0)
    turned = jnp.broadcast_to(swapped, (BOX, BOX)) == 1
    loads[0].wait()
    loads[1].wait()
    for z in range(2):
        real, imag = source[0, z], source[1, z]
        real = jnp.where(turned, real.T, real)
        imag = jnp.where(turned, imag.T, imag)
        stacked = jnp.concatenate(
            [
                jnp.concatenate([real, imag * sign_y], 1),
                jnp.concatenate([imag * sign_x, real * (-sign_x * sign_y)], 1),
            ],
            0,
        )
        along = dot3((first[0], first[1]), cut(stacked), NN)
        if z == 0:
            along = along * jnp.concatenate([row_mask, row_mask], 1)
        for c in range(2):
            base = (2 * z + c) * DEPTH
            slab_out[:, base : base + DEPTH, :] = along[:, c * 128 : (c + 1) * 128].reshape(
                PLANE, DEPTH, 128
            )
    slab_in[PLANE - 1] = slab_out[place]
    pl.semaphore_wait(barrier, PLANE + 1)

    for k, (a, b) in enumerate(plane):
        pltpu.make_async_remote_copy(
            slab_out.at[a * LINE + b, pl.ds(0, SLAB)], slab_in.at[slots[k], pl.ds(0, SLAB)],
            slab_s, slab_r.at[bunch[slots[k]]], (a * DEPTH + level, b), MESH,
        ).start()
    for step in range(3):
        pl.semaphore_signal(above_sem.at[step], 1, device_id=above, device_id_type=MESH)
        if step < 2:
            pl.semaphore_signal(below_sem.at[step], 1, device_id=below, device_id_type=MESH)
            pl.semaphore_wait(below_sem.at[step], 1)
        pl.semaphore_wait(above_sem.at[step], 1)
    kind = lax.broadcasted_iota(jnp.int32, (128, EXTENT), 0)
    ky_wide = magnitude(lax.broadcasted_iota(jnp.int32, (128, EXTENT), 1))
    reach = jnp.where(kind // 4 % 2 == 1, ky_wide, magnitude(me))
    inside_ref[...] = jnp.where(reach >= pick(kind % 4, THRESHOLDS), 1.0, 0.0).astype(bf16)
    for load in loads[5:]:
        load.wait()
    number = kind % NSHELL
    for z in range(2):
        member_ref[z] = jnp.where(number == shell[z], 1.0, 0.0).astype(bf16)

    second_pair = (second[0], second[1])
    spread_map = spread[...]
    totals = [[jnp.zeros((DEPTH, 2 * EXTENT), f32) for z in range(2)] for h in range(2)]
    counts = jnp.zeros((1, 128), f32)
    for turn_in, group in enumerate(GROUPS):
        start = sum(GROUPS[:turn_in])
        landed = slab_in.at[pl.ds(start, min(group, PLANE - 1 - start)), pl.ds(0, SLAB)]
        pltpu.make_async_copy(landed, landed, slab_r.at[turn_in]).wait()
        tags = slab_in[start : start + group, TAG, :]
        counts = counts + jnp.sum(tags, axis=0, keepdims=True)
        vectors = dot(tags.astype(bf16), spread_map, NN)
        blocks = []
        for z in range(2):
            real = slab_in[start : start + group, 2 * z * DEPTH : (2 * z + 1) * DEPTH, :]
            imag = slab_in[start : start + group, (2 * z + 1) * DEPTH : (2 * z + 2) * DEPTH, :]
            blocks.append(jnp.concatenate([real, imag], 2).reshape(group * DEPTH, EXTENT))
        waves = dot3(cut(jnp.concatenate(blocks, 0)), second_pair, NN)
        for g in range(group):
            vector = vectors[g : g + 1]
            keep = vector[:, :EXTENT]
            lane_half = jnp.concatenate([vector[:, EXTENT : EXTENT + 128]] * 4, 1)
            lane_sign = jnp.concatenate([vector[:, EXTENT + 128 :]] * 2, 1)
            factors = (
                jnp.concatenate([keep, keep * lane_sign], 1),
                jnp.concatenate([jnp.ones_like(keep), lane_sign], 1),
            )
            for z in range(2):
                base = (z * group + g) * DEPTH
                value = waves[base : base + DEPTH] * factors[z]
                upper = value * lane_half
                totals[1][z] = totals[1][z] + upper
                totals[0][z] = totals[0][z] + (value - upper)
    for h in range(2):
        for c in range(2):
            for z in range(2):
                for q in range(2):
                    base = c * EXTENT + q * 128
                    sum_out[:, q * 8 + h * 4 + c * 2 + z, :] = totals[h][z][:, base : base + 128]
    sum_out[:, SUMS - 1, :] = jnp.broadcast_to(counts, (DEPTH, 128))
    sum_in[level] = sum_out[level]

    for other in column:
        pltpu.make_async_remote_copy(
            sum_out.at[other, pl.ds(0, SUMS)], sum_in.at[level, pl.ds(0, SUMS)],
            sum_s, sum_r, (side * DEPTH + other, py), MESH,
        ).start()
    comp = lax.broadcasted_iota(jnp.int32, (8, 128), 0)
    lane = lax.broadcasted_iota(jnp.int32, (8, 128), 1)
    inside = inside_ref[...]
    members = [member_ref[0], member_ref[1]]
    landed = sum_in.at[pl.ds(0, DEPTH - 1), pl.ds(0, SUMS)]
    pltpu.make_async_copy(landed, landed, sum_r).wait()
    total = sum_in[0, :SUMS]
    for k in range(1, DEPTH):
        total = total + sum_in[k, :SUMS]
    count = total[SUMS - 1 :]
    total = jnp.concatenate([total[:8], total[8:16]], 1)
    by_half = jnp.where(lane // 8 == comp // 4, count, 0.0)
    masked_count = dot(by_half.astype(bf16), inside, NN)
    full_count = jnp.sum(by_half, axis=1, keepdims=True)
    wide_comp = lax.broadcasted_iota(jnp.int32, (8, EXTENT), 0)
    cover = jnp.where(wide_comp % 2 == 0, masked_count, full_count)
    average = total / jnp.maximum(cover, 1.0)

    powers = jnp.concatenate([average * average, average * pltpu.roll(average, 4, 0)], 0)
    powers = jnp.concatenate(cut(powers), 0)
    p_row = lax.broadcasted_iota(jnp.int32, (32, 128), 0) % 16
    p_lane = lax.broadcasted_iota(jnp.int32, (32, 128), 1)
    wanted = jnp.where(p_row < 8, 1 + p_row // 4, jnp.where(p_row < 12, 0, 4))
    part = jnp.where(p_row % 2 == 0, dot(powers, members[0], NT), dot(powers, members[1], NT))
    shells = jnp.sum(jnp.where(p_lane // NSHELL == wanted, part, 0.0), axis=0, keepdims=True)

    back_pair = (back[0], back[1])
    pair = jnp.concatenate([average, quarter_phase(average)], 1)
    middle = dot3_few(pair, back_pair)
    padded = jnp.concatenate(
        [
            jnp.zeros((MAPLANE, EXTENT), f32),
            middle,
            jnp.zeros((128 - MAPLANE - 8, EXTENT), f32),
        ],
        0,
    )
    row_out[...] = padded.T + shells
    row_in[pl.ds(me, 1)] = row_out[pl.ds(me, 1)]

    def send_row(a, c, b):
        to = (a * DEPTH + c, b)
        other = to[0] * LINE + b
        pltpu.make_async_remote_copy(
            row_out.at[pl.ds(other, 1)], row_in.at[pl.ds(me, 1)], row_s, row_r, to, MESH
        ).start()

    @pl.loop(0, DEPTH - 1)
    def _(step):
        away = lax.div(step + 1, 2)
        shift = away * (1 - 2 * lax.rem(step, 2))
        other = lax.rem(level + 12 + shift, DEPTH)
        for a, b in plane + [(side, py)]:
            send_row(a, other, b)

    for a, b in plane:
        send_row(a, level, b)

    whole = row_in.at[pl.ds(0, EXTENT - 1)]
    pltpu.make_async_copy(whole, whole, row_r).wait()
    rows = row_in[...]
    sums = jnp.sum(rows, axis=0, keepdims=True)
    values = rows.T[MAPLANE : MAPLANE + 8]
    pair = jnp.concatenate([values, quarter_phase(values)], 1)
    final = dot3_few(pair, back_pair)
    maps_ref[...] = final
    sums = jnp.broadcast_to(sums, (8, 128))
    first_power = pltpu.roll(sums, 128 - NSHELL, 1)
    second_power = pltpu.roll(sums, 128 - 2 * NSHELL, 1)
    fsc_ref[...] = sums / (jnp.sqrt(first_power * second_power) + 1e-06)

    gone = slab_out.at[pl.ds(0, PLANE - 1), pl.ds(0, SLAB)]
    pltpu.make_async_copy(gone, gone, slab_s).wait()
    pltpu.make_async_copy(landed, landed, sum_s).wait()
    pltpu.make_async_copy(whole, whole, row_s).wait()


def finish(final, shells, maps_ref, fsc_ref):
    for h in range(2):
        for c in range(2):
            for z in range(2):
                n = h * 4 + c * 2 + z
                maps_ref[h, c, z] = final[n : n + 1]
    fsc_ref[...] = shells[0, :NSHELL]


def shards(particles, orientation, wedge_index, half_set, shell_map):
    first, second, back, spread = tables()
    first, second, back = (halves(t) for t in (first, second, back))
    spread = jnp.asarray(spread, bf16)
    vmem = pl.BlockSpec(memory_space=pltpu.VMEM)
    hbm = pl.BlockSpec(memory_space=pltpu.HBM)
    dma = pltpu.SemaphoreType.DMA
    final, shells = pl.pallas_call(
        body,
        out_shape=(
            pltpu.VMEM((8, EXTENT), f32),
            pltpu.VMEM((8, 128), f32),
        ),
        in_specs=[hbm] * 9,
        out_specs=(vmem, vmem),
        scratch_shapes=[
            pltpu.SMEM((1,), jnp.int32), pltpu.SMEM((1,), jnp.int32), pltpu.SMEM((1,), jnp.int32),
            pltpu.VMEM((2, 2, BOX, BOX), f32),
            pltpu.VMEM((2, 1, EXTENT), jnp.int32),
            pltpu.VMEM((2, EXTENT, EXTENT), bf16),
            pltpu.VMEM((2, EXTENT, 2 * EXTENT), bf16),
            pltpu.VMEM((2, 2 * EXTENT, EXTENT), bf16),
            pltpu.VMEM((128, 2 * EXTENT), bf16),
            pltpu.VMEM((PLANE, SLAB + 7, 128), f32),
            pltpu.VMEM((PLANE, SLAB + 7, 128), f32),
            pltpu.VMEM((DEPTH, SUMS + 7, 128), f32),
            pltpu.VMEM((DEPTH, SUMS + 7, 128), f32),
            pltpu.VMEM((EXTENT, 128), f32),
            pltpu.VMEM((EXTENT, 128), f32),
            pltpu.VMEM((128, EXTENT), bf16),
            pltpu.VMEM((2, 128, EXTENT), bf16),
            dma((9,)),
            dma, dma((len(GROUPS),)), dma, dma, dma, dma,
            pltpu.SemaphoreType.REGULAR((3,)), pltpu.SemaphoreType.REGULAR((2,)),
        ],
        compiler_params=pltpu.CompilerParams(collective_id=0, has_side_effects=True),
        name="subtomogram_average",
    )(
        orientation, wedge_index, half_set, particles[0], shell_map, first, second, back, spread
    )
    final = pltpu.with_memory_space_constraint(final, pltpu.VMEM)
    shells = pltpu.with_memory_space_constraint(shells, pltpu.VMEM)
    return pl.pallas_call(
        finish,
        out_shape=(
            jax.ShapeDtypeStruct((2, 2, 2, 1, EXTENT), f32),
            jax.ShapeDtypeStruct((NSHELL,), f32),
        ),
        in_specs=[vmem, vmem],
        out_specs=(vmem, vmem),
        name="hand_out",
    )(final, shells)


def solution(mesh):
    both = ("px", "py")
    return jax.shard_map(
        shards,
        mesh=mesh,
        in_specs=(P(both, None, None, None, None), P(both), P(both), P(both), P(None, both, None)),
        out_specs=(P(None, None, None, both, None), P()),
        check_vma=False,
    )
```

```python
import functools
import math

import jax
import jax.numpy as jnp
import numpy as np
from jax import lax
from jax.experimental import pallas as pl
from jax.experimental.pallas import tpu as pltpu
from jax.sharding import PartitionSpec as P

RISE = (1, 3, 2, 3)
RUN = (1, 2, 1, 1)
NSHELL = 32
PLANE = 32
DEPTH = 8
LINE = 16
EXTENT = 256
BOX = 128
KZ = 128
THRESHOLDS = tuple(-(-KZ * run // rise) for rise, run in zip(RISE, RUN))
MESH = pl.DeviceIdType.MESH
f32 = jnp.float32
bf16 = jnp.bfloat16
NT = (((1,), (1,)), ((), ()))
NN = (((1,), (0,)), ((), ()))
MAPLANE = 96
GROUPS = (8, 8, 8, 8)
SUMS = 17
TAG = 2 * 2 * DEPTH
SLAB = TAG + 1
SIGN = 16


def halves(table):
    table = jnp.asarray(table, f32)
    upper = table.astype(bf16)
    lower = (table - upper.astype(f32)).astype(bf16)
    return jnp.stack([upper, lower])


def tables():
    freq = np.arange(EXTENT)
    cell = np.arange(BOX) - BOX // 2
    scale = 1.0 / math.sqrt(EXTENT)
    unit = 2.0 * math.pi / EXTENT
    place, level = np.arange(PLANE)[:, None], np.arange(DEPTH)[None, :]
    order = (place // LINE * (LINE * DEPTH) + level * LINE + place % LINE).reshape(-1)
    angle = (order[:, None] * cell[None, :] % EXTENT) * unit
    first = np.concatenate([np.cos(angle), np.sin(angle)], 1) * scale
    angle = (cell[:, None] * freq[None, :] % EXTENT) * unit
    cosine, sine = np.cos(angle) * scale, np.sin(angle) * scale
    second = np.block([[cosine, -sine], [sine, cosine]])
    angle = (freq[:, None] * freq[None, :] % EXTENT) * unit
    back = np.concatenate([np.cos(angle), np.sin(angle)], 0) * scale
    spread = np.zeros((128, 2 * EXTENT), np.float32)
    size = np.minimum(freq, EXTENT - freq)
    for kind in range(SIGN):
        keep = size >= THRESHOLDS[kind % 4] if kind // 4 % 2 else size >= 0
        spread[kind, :EXTENT] = keep
        spread[kind, EXTENT : EXTENT + 128] = kind // 8
    spread[SIGN, EXTENT + 128 :] = 1.0
    return [np.asarray(t, np.float32) for t in (first, second, back, spread)]


def cut(value):
    upper = value.astype(bf16)
    return upper, (value - upper.astype(f32)).astype(bf16)


def dot(a, b, dims):
    return lax.dot_general(a, b, dims, preferred_element_type=f32)


def dot3(a, b, dims):
    return dot(a[0], b[0], dims) + (dot(a[0], b[1], dims) + dot(a[1], b[0], dims))


def dot3_few(a, b):
    rows = a.shape[0]
    upper, lower = cut(a)
    both = dot(jnp.concatenate([upper, lower], 0), b[0], NN)
    return both[:rows] + (both[rows:] + dot(upper, b[1], NN))


def magnitude(index):
    return jnp.minimum(index, EXTENT - index)


def pick(position, entries):
    result = jnp.full_like(position, entries[0])
    for number, entry in enumerate(entries[1:], 1):
        result = jnp.where(position == number, entry, result)
    return result


def quarter_phase(value):
    row = lax.broadcasted_iota(jnp.int32, value.shape, 0)
    return jnp.where(row // 2 % 2 == 0, -pltpu.roll(value, 6, 0), pltpu.roll(value, 2, 0))


def body(
    orient_t, wedge_t, half_t, particle, shell_t, first_t, second_t, back_t, spread_t,
    maps_ref, fsc_ref,
    orient, wedge, half, source, shell, first, second, back, spread, slab_out, slab_in,
    sum_out, sum_in, row_out, row_in, inside_ref, member_ref,
    load_sem, slab_s, slab_r, sum_s, sum_r, row_s, row_r,
    above_sem, below_sem,
):
    px, py = lax.axis_index("px"), lax.axis_index("py")
    me = px * LINE + py
    side, level = lax.div(px, DEPTH), lax.rem(px, DEPTH)
    place = side * LINE + py
    y = lax.div(py, 4)
    ys = [y] + [lax.rem(y + b, 4) for b in range(1, 4)]
    near_bit, core = lax.rem(lax.div(py, 2), 2), lax.rem(py, 2)
    low = [near_bit * 2 + core, near_bit * 2 + 1 - core]
    low += [2 - near_bit * 2 + core, 3 - near_bit * 2 - core]
    sides = [side, 1 - side]
    offsets = [(1, 2, 1), (1, 2, 0), (0, 2, 3), (1, 1, 1), (1, 2, 3), (1, 3, 1), (0, 2, 2), (1, 1, 0), (1, 2, 2), (1, 3, 0), (0, 1, 3), (0, 2, 1), (0, 3, 3), (1, 0, 1), (1, 1, 3), (1, 3, 3), (0, 1, 2), (0, 2, 0), (0, 3, 2), (1, 0, 0), (1, 1, 2), (1, 3, 2), (0, 0, 3), (0, 1, 1), (0, 3, 1), (1, 0, 3), (0, 0, 2), (0, 1, 0), (0, 3, 0), (1, 0, 2), (0, 0, 1)]
    bunch = [n for n, size in enumerate(GROUPS) for _ in range(size)]
    plane = [(sides[a], ys[b] * 4 + low[c]) for a, b, c in offsets]
    slots = [offsets.index((a, (4 - b) % 4, c)) for a, b, c in offsets]
    levels = [level] + [lax.rem(level + c, DEPTH) for c in range(1, DEPTH)]
    column = [levels[c] for c in (4, 3, 5, 2, 6, 1, 7)]
    above, further_up = (side * DEPTH + levels[1], py), (side * DEPTH + levels[2], py)
    below, further_down = (side * DEPTH + levels[7], py), (side * DEPTH + levels[6], py)
    pairs = [
        (particle, source), (first_t, first), (orient_t, orient), (wedge_t, wedge),
        (half_t, half), (second_t, second), (spread_t, spread), (shell_t, shell), (back_t, back),
    ]
    loads = [pltpu.make_async_copy(a, b, load_sem.at[i]) for i, (a, b) in enumerate(pairs)]
    barrier = pltpu.get_barrier_semaphore()
    for a, b in plane:
        pl.semaphore_signal(barrier, 1, device_id=(a * DEPTH + level, b), device_id_type=MESH)
    for neighbour in (further_up, further_down, above, below):
        pl.semaphore_signal(barrier, 1, device_id=neighbour, device_id_type=MESH)

    for load in loads:
        load.start()
    for load in loads[2:5]:
        load.wait()
    turn, wedge_id, half_id = orient[0], wedge[0], half[0]
    quarter = turn % 4
    sign_x = (1 - 2 * ((quarter + 1) // 2 % 2)).astype(f32)
    sign_y = ((1 - 2 * (quarter // 2)) * (1 - 2 * (turn // 4))).astype(f32)
    swapped = turn % 2

    lane = lax.broadcasted_iota(jnp.int32, (PLANE, 128), 1)
    own_class = half_id * 8 + swapped * 4 + wedge_id
    tag = jnp.where(lane == own_class, 1.0, 0.0)
    tag = jnp.where(lane == SIGN, jnp.broadcast_to(sign_y, (PLANE, 128)), tag)
    slab_out[:, TAG, :] = tag

    row = lax.broadcasted_iota(jnp.int32, (EXTENT, 128), 0)
    kx = row // (DEPTH * LINE) * (DEPTH * LINE) + row % DEPTH * LINE + row // DEPTH % LINE
    kx_abs = magnitude(kx)
    row_limit = pick(jnp.broadcast_to(wedge_id, (EXTENT, 128)), THRESHOLDS) * (1 - swapped)
    row_mask = jnp.where(kx_abs >= row_limit, 1.0, 0.0)
    turned = jnp.broadcast_to(swapped, (BOX, BOX)) == 1
    loads[0].wait()
    loads[1].wait()
    for z in range(2):
        real, imag = source[0, z], source[1, z]
        real = jnp.where(turned, real.T, real)
        imag = jnp.where(turned, imag.T, imag)
        stacked = jnp.concatenate(
            [
                jnp.concatenate([real, imag * sign_y], 1),
                jnp.concatenate([imag * sign_x, real * (-sign_x * sign_y)], 1),
            ],
            0,
        )
        along = dot3((first[0], first[1]), cut(stacked), NN)
        if z == 0:
            along = along * jnp.concatenate([row_mask, row_mask], 1)
        for c in range(2):
            base = (2 * z + c) * DEPTH
            slab_out[:, base : base + DEPTH, :] = along[:, c * 128 : (c + 1) * 128].reshape(
                PLANE, DEPTH, 128
            )
    slab_in[PLANE - 1] = slab_out[place]
    pl.semaphore_wait(barrier, PLANE + 3)

    for k, (a, b) in enumerate(plane):
        pltpu.make_async_remote_copy(
            slab_out.at[a * LINE + b, pl.ds(0, SLAB)], slab_in.at[slots[k], pl.ds(0, SLAB)],
            slab_s, slab_r.at[bunch[slots[k]]], (a * DEPTH + level, b), MESH,
        ).start()
    pl.semaphore_signal(above_sem, 1, device_id=further_up, device_id_type=MESH)
    pl.semaphore_signal(below_sem, 1, device_id=further_down, device_id_type=MESH)

    kind = lax.broadcasted_iota(jnp.int32, (128, EXTENT), 0)
    ky_wide = magnitude(lax.broadcasted_iota(jnp.int32, (128, EXTENT), 1))
    reach = jnp.where(kind // 4 % 2 == 1, ky_wide, magnitude(me))
    inside_ref[...] = jnp.where(reach >= pick(kind % 4, THRESHOLDS), 1.0, 0.0).astype(bf16)
    for load in loads[5:]:
        load.wait()
    number = kind % NSHELL
    for z in range(2):
        member_ref[z] = jnp.where(number == shell[z], 1.0, 0.0).astype(bf16)

    second_pair = (second[0], second[1])
    spread_map = spread[...]
    totals = [[jnp.zeros((DEPTH, 2 * EXTENT), f32) for z in range(2)] for h in range(2)]
    counts = jnp.zeros((1, 128), f32)
    for turn_in, group in enumerate(GROUPS):
        start = sum(GROUPS[:turn_in])
        landed = slab_in.at[pl.ds(start, min(group, PLANE - 1 - start)), pl.ds(0, SLAB)]
        pltpu.make_async_copy(landed, landed, slab_r.at[turn_in]).wait()
        tags = slab_in[start : start + group, TAG, :]
        counts = counts + jnp.sum(tags, axis=0, keepdims=True)
        vectors = dot(tags.astype(bf16), spread_map, NN)
        blocks = []
        for z in range(2):
            real = slab_in[start : start + group, 2 * z * DEPTH : (2 * z + 1) * DEPTH, :]
            imag = slab_in[start : start + group, (2 * z + 1) * DEPTH : (2 * z + 2) * DEPTH, :]
            blocks.append(jnp.concatenate([real, imag], 2).reshape(group * DEPTH, EXTENT))
        waves = dot3(cut(jnp.concatenate(blocks, 0)), second_pair, NN)
        for g in range(group):
            vector = vectors[g : g + 1]
            keep = vector[:, :EXTENT]
            lane_half = jnp.concatenate([vector[:, EXTENT : EXTENT + 128]] * 4, 1)
            lane_sign = jnp.concatenate([vector[:, EXTENT + 128 :]] * 2, 1)
            factors = (
                jnp.concatenate([keep, keep * lane_sign], 1),
                jnp.concatenate([jnp.ones_like(keep), lane_sign], 1),
            )
            for z in range(2):
                base = (z * group + g) * DEPTH
                value = waves[base : base + DEPTH] * factors[z]
                upper = value * lane_half
                totals[1][z] = totals[1][z] + upper
                totals[0][z] = totals[0][z] + (value - upper)
    for h in range(2):
        for c in range(2):
            for z in range(2):
                for q in range(2):
                    base = c * EXTENT + q * 128
                    sum_out[:, q * 8 + h * 4 + c * 2 + z, :] = totals[h][z][:, base : base + 128]
    sum_out[:, SUMS - 1, :] = jnp.broadcast_to(counts, (DEPTH, 128))
    sum_in[level] = sum_out[level]

    pl.semaphore_wait(above_sem, 1)
    pl.semaphore_wait(below_sem, 1)
    for other in column:
        pltpu.make_async_remote_copy(
            sum_out.at[other, pl.ds(0, SUMS)], sum_in.at[level, pl.ds(0, SUMS)],
            sum_s, sum_r, (side * DEPTH + other, py), MESH,
        ).start()
    comp = lax.broadcasted_iota(jnp.int32, (8, 128), 0)
    lane = lax.broadcasted_iota(jnp.int32, (8, 128), 1)
    inside = inside_ref[...]
    members = [member_ref[0], member_ref[1]]
    landed = sum_in.at[pl.ds(0, DEPTH - 1), pl.ds(0, SUMS)]
    pltpu.make_async_copy(landed, landed, sum_r).wait()
    total = sum_in[0, :SUMS]
    for k in range(1, DEPTH):
        total = total + sum_in[k, :SUMS]
    count = total[SUMS - 1 :]
    total = jnp.concatenate([total[:8], total[8:16]], 1)
    by_half = jnp.where(lane // 8 == comp // 4, count, 0.0)
    masked_count = dot(by_half.astype(bf16), inside, NN)
    full_count = jnp.sum(by_half, axis=1, keepdims=True)
    wide_comp = lax.broadcasted_iota(jnp.int32, (8, EXTENT), 0)
    cover = jnp.where(wide_comp % 2 == 0, masked_count, full_count)
    average = total / jnp.maximum(cover, 1.0)

    powers = jnp.concatenate([average * average, average * pltpu.roll(average, 4, 0)], 0)
    powers = jnp.concatenate(cut(powers), 0)
    p_row = lax.broadcasted_iota(jnp.int32, (32, 128), 0) % 16
    p_lane = lax.broadcasted_iota(jnp.int32, (32, 128), 1)
    wanted = jnp.where(p_row < 8, 1 + p_row // 4, jnp.where(p_row < 12, 0, 4))
    part = jnp.where(p_row % 2 == 0, dot(powers, members[0], NT), dot(powers, members[1], NT))
    shells = jnp.sum(jnp.where(p_lane // NSHELL == wanted, part, 0.0), axis=0, keepdims=True)

    back_pair = (back[0], back[1])
    pair = jnp.concatenate([average, quarter_phase(average)], 1)
    middle = dot3_few(pair, back_pair)
    padded = jnp.concatenate(
        [
            jnp.zeros((MAPLANE, EXTENT), f32),
            middle,
            jnp.zeros((128 - MAPLANE - 8, EXTENT), f32),
        ],
        0,
    )
    row_out[...] = padded.T + shells
    row_in[pl.ds(me, 1)] = row_out[pl.ds(me, 1)]

    def send_row(a, c, b):
        to = (a * DEPTH + c, b)
        other = to[0] * LINE + b
        pltpu.make_async_remote_copy(
            row_out.at[pl.ds(other, 1)], row_in.at[pl.ds(me, 1)], row_s, row_r, to, MESH
        ).start()

    @pl.loop(0, DEPTH - 1)
    def _(step):
        away = lax.div(step + 1, 2)
        shift = away * (1 - 2 * lax.rem(step, 2))
        other = lax.rem(level + 12 + shift, DEPTH)
        for a, b in plane + [(side, py)]:
            send_row(a, other, b)

    for a, b in plane:
        send_row(a, level, b)

    whole = row_in.at[pl.ds(0, EXTENT - 1)]
    pltpu.make_async_copy(whole, whole, row_r).wait()
    rows = row_in[...]
    sums = jnp.sum(rows, axis=0, keepdims=True)
    values = rows.T[MAPLANE : MAPLANE + 8]
    pair = jnp.concatenate([values, quarter_phase(values)], 1)
    final = dot3_few(pair, back_pair)
    maps_ref[...] = final
    sums = jnp.broadcast_to(sums, (8, 128))
    first_power = pltpu.roll(sums, 128 - NSHELL, 1)
    second_power = pltpu.roll(sums, 128 - 2 * NSHELL, 1)
    fsc_ref[...] = sums / (jnp.sqrt(first_power * second_power) + 1e-06)

    gone = slab_out.at[pl.ds(0, PLANE - 1), pl.ds(0, SLAB)]
    pltpu.make_async_copy(gone, gone, slab_s).wait()
    pltpu.make_async_copy(landed, landed, sum_s).wait()
    pltpu.make_async_copy(whole, whole, row_s).wait()


def finish(final, shells, maps_ref, fsc_ref):
    for h in range(2):
        for c in range(2):
            for z in range(2):
                n = h * 4 + c * 2 + z
                maps_ref[h, c, z] = final[n : n + 1]
    fsc_ref[...] = shells[0, :NSHELL]


def shards(particles, orientation, wedge_index, half_set, shell_map):
    first, second, back, spread = tables()
    first, second, back = (halves(t) for t in (first, second, back))
    spread = jnp.asarray(spread, bf16)
    vmem = pl.BlockSpec(memory_space=pltpu.VMEM)
    hbm = pl.BlockSpec(memory_space=pltpu.HBM)
    dma = pltpu.SemaphoreType.DMA
    final, shells = pl.pallas_call(
        body,
        out_shape=(
            pltpu.VMEM((8, EXTENT), f32),
            pltpu.VMEM((8, 128), f32),
        ),
        in_specs=[hbm] * 9,
        out_specs=(vmem, vmem),
        scratch_shapes=[
            pltpu.SMEM((1,), jnp.int32), pltpu.SMEM((1,), jnp.int32), pltpu.SMEM((1,), jnp.int32),
            pltpu.VMEM((2, 2, BOX, BOX), f32),
            pltpu.VMEM((2, 1, EXTENT), jnp.int32),
            pltpu.VMEM((2, EXTENT, EXTENT), bf16),
            pltpu.VMEM((2, EXTENT, 2 * EXTENT), bf16),
            pltpu.VMEM((2, 2 * EXTENT, EXTENT), bf16),
            pltpu.VMEM((128, 2 * EXTENT), bf16),
            pltpu.VMEM((PLANE, SLAB + 7, 128), f32),
            pltpu.VMEM((PLANE, SLAB + 7, 128), f32),
            pltpu.VMEM((DEPTH, SUMS + 7, 128), f32),
            pltpu.VMEM((DEPTH, SUMS + 7, 128), f32),
            pltpu.VMEM((EXTENT, 128), f32),
            pltpu.VMEM((EXTENT, 128), f32),
            pltpu.VMEM((128, EXTENT), bf16),
            pltpu.VMEM((2, 128, EXTENT), bf16),
            dma((9,)),
            dma, dma((len(GROUPS),)), dma, dma, dma, dma,
            pltpu.SemaphoreType.REGULAR, pltpu.SemaphoreType.REGULAR,
        ],
        compiler_params=pltpu.CompilerParams(
            collective_id=0, has_side_effects=True,
        ),
        name="subtomogram_average",
    )(
        orientation, wedge_index, half_set, particles[0], shell_map, first, second, back, spread
    )
    final = pltpu.with_memory_space_constraint(final, pltpu.VMEM)
    shells = pltpu.with_memory_space_constraint(shells, pltpu.VMEM)
    return pl.pallas_call(
        finish,
        out_shape=(
            jax.ShapeDtypeStruct((2, 2, 2, 1, EXTENT), f32),
            jax.ShapeDtypeStruct((NSHELL,), f32),
        ),
        in_specs=[vmem, vmem],
        out_specs=(vmem, vmem),
        name="hand_out",
    )(final, shells)


def solution(mesh):
    both = ("px", "py")
    return jax.shard_map(
        shards,
        mesh=mesh,
        in_specs=(P(both, None, None, None, None), P(both), P(both), P(both), P(None, both, None)),
        out_specs=(P(None, None, None, both, None), P()),
        check_vma=False,
    )
```

```python
import functools
import math

import jax
import jax.numpy as jnp
import numpy as np
from jax import lax
from jax.experimental import pallas as pl
from jax.experimental.pallas import tpu as pltpu
from jax.sharding import PartitionSpec as P

RISE = (1, 3, 2, 3)
RUN = (1, 2, 1, 1)
NSHELL = 32
PLANE = 32
DEPTH = 8
LINE = 16
EXTENT = 256
BOX = 128
KZ = 128
THRESHOLDS = tuple(-(-KZ * run // rise) for rise, run in zip(RISE, RUN))
MESH = pl.DeviceIdType.MESH
f32 = jnp.float32
bf16 = jnp.bfloat16
NT = (((1,), (1,)), ((), ()))
NN = (((1,), (0,)), ((), ()))
MAPLANE = 96
GROUPS = (8, 8, 8, 8)
SUMS = 17
TAG = 2 * 2 * DEPTH
SLAB = TAG + 1
SIGN = 16


def halves(table):
    table = jnp.asarray(table, f32)
    upper = table.astype(bf16)
    lower = (table - upper.astype(f32)).astype(bf16)
    return jnp.stack([upper, lower])


def tables():
    freq = np.arange(EXTENT)
    cell = np.arange(BOX) - BOX // 2
    scale = 1.0 / math.sqrt(EXTENT)
    unit = 2.0 * math.pi / EXTENT
    place, level = np.arange(PLANE)[:, None], np.arange(DEPTH)[None, :]
    order = (place // LINE * (LINE * DEPTH) + level * LINE + place % LINE).reshape(-1)
    angle = (order[:, None] * cell[None, :] % EXTENT) * unit
    first = np.concatenate([np.cos(angle), np.sin(angle)], 1) * scale
    angle = (cell[:, None] * freq[None, :] % EXTENT) * unit
    cosine, sine = np.cos(angle) * scale, np.sin(angle) * scale
    second = np.block([[cosine, -sine], [sine, cosine]])
    angle = (freq[:, None] * freq[None, :] % EXTENT) * unit
    back = np.concatenate([np.cos(angle), np.sin(angle)], 0) * scale
    spread = np.zeros((128, 2 * EXTENT), np.float32)
    size = np.minimum(freq, EXTENT - freq)
    for kind in range(SIGN):
        keep = size >= THRESHOLDS[kind % 4] if kind // 4 % 2 else size >= 0
        spread[kind, :EXTENT] = keep
        spread[kind, EXTENT : EXTENT + 128] = kind // 8
    spread[SIGN, EXTENT + 128 :] = 1.0
    return [np.asarray(t, np.float32) for t in (first, second, back, spread)]


def cut(value):
    upper = value.astype(bf16)
    return upper, (value - upper.astype(f32)).astype(bf16)


def dot(a, b, dims):
    return lax.dot_general(a, b, dims, preferred_element_type=f32)


def dot3(a, b, dims):
    return dot(a[0], b[0], dims) + (dot(a[0], b[1], dims) + dot(a[1], b[0], dims))


def dot3_few(a, b):
    rows = a.shape[0]
    upper, lower = cut(a)
    both = dot(jnp.concatenate([upper, lower], 0), b[0], NN)
    return both[:rows] + (both[rows:] + dot(upper, b[1], NN))


def magnitude(index):
    return jnp.minimum(index, EXTENT - index)


def pick(position, entries):
    result = jnp.full_like(position, entries[0])
    for number, entry in enumerate(entries[1:], 1):
        result = jnp.where(position == number, entry, result)
    return result


def quarter_phase(value):
    row = lax.broadcasted_iota(jnp.int32, value.shape, 0)
    return jnp.where(row // 2 % 2 == 0, -pltpu.roll(value, 6, 0), pltpu.roll(value, 2, 0))


def body(
    orient_t, wedge_t, half_t, particle, shell_t, first_t, second_t, back_t, spread_t,
    maps_ref, fsc_ref,
    orient, wedge, half, source, shell, first, second, back, spread, slab_out, slab_in,
    sum_out, sum_in, row_out, row_in, inside_ref, member_ref,
    load_sem, slab_s, slab_r, sum_s, sum_r, row_s, row_r,
    above_sem, below_sem,
):
    px, py = lax.axis_index("px"), lax.axis_index("py")
    me = px * LINE + py
    side, level = lax.div(px, DEPTH), lax.rem(px, DEPTH)
    place = side * LINE + py
    y = lax.div(py, 4)
    ys = [y] + [lax.rem(y + b, 4) for b in range(1, 4)]
    near_bit, core = lax.rem(lax.div(py, 2), 2), lax.rem(py, 2)
    low = [near_bit * 2 + core, near_bit * 2 + 1 - core]
    low += [2 - near_bit * 2 + core, 3 - near_bit * 2 - core]
    sides = [side, 1 - side]
    offsets = [(1, 2, 1), (1, 2, 0), (0, 2, 3), (1, 1, 1), (1, 2, 3), (1, 3, 1), (0, 2, 2), (1, 1, 0), (1, 2, 2), (1, 3, 0), (0, 1, 3), (0, 2, 1), (0, 3, 3), (1, 0, 1), (1, 1, 3), (1, 3, 3), (0, 1, 2), (0, 2, 0), (0, 3, 2), (1, 0, 0), (1, 1, 2), (1, 3, 2), (0, 0, 3), (0, 1, 1), (0, 3, 1), (1, 0, 3), (0, 0, 2), (0, 1, 0), (0, 3, 0), (1, 0, 2), (0, 0, 1)]
    bunch = [n for n, size in enumerate(GROUPS) for _ in range(size)]
    plane = [(sides[a], ys[b] * 4 + low[c]) for a, b, c in offsets]
    slots = [offsets.index((a, (4 - b) % 4, c)) for a, b, c in offsets]
    levels = [level] + [lax.rem(level + c, DEPTH) for c in range(1, DEPTH)]
    column = [levels[c] for c in (4, 3, 5, 2, 6, 1, 7)]
    above = (side * DEPTH + levels[1], py)
    below = (side * DEPTH + levels[7], py)
    pairs = [
        (particle, source), (first_t, first), (orient_t, orient), (wedge_t, wedge),
        (half_t, half), (second_t, second), (spread_t, spread), (shell_t, shell), (back_t, back),
    ]
    loads = [pltpu.make_async_copy(a, b, load_sem.at[i]) for i, (a, b) in enumerate(pairs)]
    barrier = pltpu.get_barrier_semaphore()
    for a, b in plane:
        pl.semaphore_signal(barrier, 1, device_id=(a * DEPTH + level, b), device_id_type=MESH)
    for neighbour in (above, below):
        pl.semaphore_signal(barrier, 1, device_id=neighbour, device_id_type=MESH)

    for load in loads:
        load.start()
    for load in loads[2:5]:
        load.wait()
    turn, wedge_id, half_id = orient[0], wedge[0], half[0]
    quarter = turn % 4
    sign_x = (1 - 2 * ((quarter + 1) // 2 % 2)).astype(f32)
    sign_y = ((1 - 2 * (quarter // 2)) * (1 - 2 * (turn // 4))).astype(f32)
    swapped = turn % 2

    lane = lax.broadcasted_iota(jnp.int32, (PLANE, 128), 1)
    own_class = half_id * 8 + swapped * 4 + wedge_id
    tag = jnp.where(lane == own_class, 1.0, 0.0)
    tag = jnp.where(lane == SIGN, jnp.broadcast_to(sign_y, (PLANE, 128)), tag)
    slab_out[:, TAG, :] = tag

    row = lax.broadcasted_iota(jnp.int32, (EXTENT, 128), 0)
    kx = row // (DEPTH * LINE) * (DEPTH * LINE) + row % DEPTH * LINE + row // DEPTH % LINE
    kx_abs = magnitude(kx)
    row_limit = pick(jnp.broadcast_to(wedge_id, (EXTENT, 128)), THRESHOLDS) * (1 - swapped)
    row_mask = jnp.where(kx_abs >= row_limit, 1.0, 0.0)
    turned = jnp.broadcast_to(swapped, (BOX, BOX)) == 1
    loads[0].wait()
    loads[1].wait()
    for z in range(2):
        real, imag = source[0, z], source[1, z]
        real = jnp.where(turned, real.T, real)
        imag = jnp.where(turned, imag.T, imag)
        stacked = jnp.concatenate(
            [
                jnp.concatenate([real, imag * sign_y], 1),
                jnp.concatenate([imag * sign_x, real * (-sign_x * sign_y)], 1),
            ],
            0,
        )
        along = dot3((first[0], first[1]), cut(stacked), NN)
        if z == 0:
            along = along * jnp.concatenate([row_mask, row_mask], 1)
        for c in range(2):
            base = (2 * z + c) * DEPTH
            slab_out[:, base : base + DEPTH, :] = along[:, c * 128 : (c + 1) * 128].reshape(
                PLANE, DEPTH, 128
            )
    slab_in[PLANE - 1] = slab_out[place]
    pl.semaphore_wait(barrier, PLANE + 1)

    for k, (a, b) in enumerate(plane):
        pltpu.make_async_remote_copy(
            slab_out.at[a * LINE + b, pl.ds(0, SLAB)], slab_in.at[slots[k], pl.ds(0, SLAB)],
            slab_s, slab_r.at[bunch[slots[k]]], (a * DEPTH + level, b), MESH,
        ).start()
    for step in range(3):
        pl.semaphore_signal(above_sem.at[step], 1, device_id=above, device_id_type=MESH)
        if step < 2:
            pl.semaphore_signal(below_sem.at[step], 1, device_id=below, device_id_type=MESH)
            pl.semaphore_wait(below_sem.at[step], 1)
        pl.semaphore_wait(above_sem.at[step], 1)
    kind = lax.broadcasted_iota(jnp.int32, (128, EXTENT), 0)
    ky_wide = magnitude(lax.broadcasted_iota(jnp.int32, (128, EXTENT), 1))
    reach = jnp.where(kind // 4 % 2 == 1, ky_wide, magnitude(me))
    inside_ref[...] = jnp.where(reach >= pick(kind % 4, THRESHOLDS), 1.0, 0.0).astype(bf16)
    for load in loads[5:]:
        load.wait()
    number = kind % NSHELL
    for z in range(2):
        member_ref[z] = jnp.where(number == shell[z], 1.0, 0.0).astype(bf16)

    second_pair = (second[0], second[1])
    spread_map = spread[...]
    totals = [[jnp.zeros((DEPTH, 2 * EXTENT), f32) for z in range(2)] for h in range(2)]
    counts = jnp.zeros((1, 128), f32)
    for turn_in, group in enumerate(GROUPS):
        start = sum(GROUPS[:turn_in])
        landed = slab_in.at[pl.ds(start, min(group, PLANE - 1 - start)), pl.ds(0, SLAB)]
        pltpu.make_async_copy(landed, landed, slab_r.at[turn_in]).wait()
        tags = slab_in[start : start + group, TAG, :]
        counts = counts + jnp.sum(tags, axis=0, keepdims=True)
        vectors = dot(tags.astype(bf16), spread_map, NN)
        blocks = []
        for z in range(2):
            real = slab_in[start : start + group, 2 * z * DEPTH : (2 * z + 1) * DEPTH, :]
            imag = slab_in[start : start + group, (2 * z + 1) * DEPTH : (2 * z + 2) * DEPTH, :]
            blocks.append(jnp.concatenate([real, imag], 2).reshape(group * DEPTH, EXTENT))
        waves = dot3(cut(jnp.concatenate(blocks, 0)), second_pair, NN)
        for g in range(group):
            vector = vectors[g : g + 1]
            keep = vector[:, :EXTENT]
            lane_half = jnp.concatenate([vector[:, EXTENT : EXTENT + 128]] * 4, 1)
            lane_sign = jnp.concatenate([vector[:, EXTENT + 128 :]] * 2, 1)
            factors = (
                jnp.concatenate([keep, keep * lane_sign], 1),
                jnp.concatenate([jnp.ones_like(keep), lane_sign], 1),
            )
            for z in range(2):
                base = (z * group + g) * DEPTH
                value = waves[base : base + DEPTH] * factors[z]
                upper = value * lane_half
                totals[1][z] = totals[1][z] + upper
                totals[0][z] = totals[0][z] + (value - upper)
    for h in range(2):
        for c in range(2):
            for z in range(2):
                for q in range(2):
                    base = c * EXTENT + q * 128
                    sum_out[:, q * 8 + h * 4 + c * 2 + z, :] = totals[h][z][:, base : base + 128]
    sum_out[:, SUMS - 1, :] = jnp.broadcast_to(counts, (DEPTH, 128))
    sum_in[level] = sum_out[level]

    for other in column:
        pltpu.make_async_remote_copy(
            sum_out.at[other, pl.ds(0, SUMS)], sum_in.at[level, pl.ds(0, SUMS)],
            sum_s, sum_r, (side * DEPTH + other, py), MESH,
        ).start()
    comp = lax.broadcasted_iota(jnp.int32, (8, 128), 0)
    lane = lax.broadcasted_iota(jnp.int32, (8, 128), 1)
    inside = inside_ref[...]
    members = [member_ref[0], member_ref[1]]
    landed = sum_in.at[pl.ds(0, DEPTH - 1), pl.ds(0, SUMS)]
    pltpu.make_async_copy(landed, landed, sum_r).wait()
    total = sum_in[0, :SUMS]
    for k in range(1, DEPTH):
        total = total + sum_in[k, :SUMS]
    count = total[SUMS - 1 :]
    total = jnp.concatenate([total[:8], total[8:16]], 1)
    by_half = jnp.where(lane // 8 == comp // 4, count, 0.0)
    masked_count = dot(by_half.astype(bf16), inside, NN)
    full_count = jnp.sum(by_half, axis=1, keepdims=True)
    wide_comp = lax.broadcasted_iota(jnp.int32, (8, EXTENT), 0)
    cover = jnp.where(wide_comp % 2 == 0, masked_count, full_count)
    average = total / jnp.maximum(cover, 1.0)

    powers = jnp.concatenate([average * average, average * pltpu.roll(average, 4, 0)], 0)
    powers = jnp.concatenate(cut(powers), 0)
    p_row = lax.broadcasted_iota(jnp.int32, (32, 128), 0) % 16
    p_lane = lax.broadcasted_iota(jnp.int32, (32, 128), 1)
    wanted = jnp.where(p_row < 8, 1 + p_row // 4, jnp.where(p_row < 12, 0, 4))
    part = jnp.where(p_row % 2 == 0, dot(powers, members[0], NT), dot(powers, members[1], NT))
    shells = jnp.sum(jnp.where(p_lane // NSHELL == wanted, part, 0.0), axis=0, keepdims=True)

    back_pair = (back[0], back[1])
    pair = jnp.concatenate([average, quarter_phase(average)], 1)
    middle = dot3_few(pair, back_pair)
    padded = jnp.concatenate(
        [
            jnp.zeros((MAPLANE, EXTENT), f32),
            middle,
            jnp.zeros((128 - MAPLANE - 8, EXTENT), f32),
        ],
        0,
    )
    row_out[...] = padded.T + shells
    row_in[pl.ds(me, 1)] = row_out[pl.ds(me, 1)]

    def send_row(a, c, b):
        to = (a * DEPTH + c, b)
        other = to[0] * LINE + b
        pltpu.make_async_remote_copy(
            row_out.at[pl.ds(other, 1)], row_in.at[pl.ds(me, 1)], row_s, row_r, to, MESH
        ).start()

    @pl.loop(0, DEPTH - 1)
    def _(step):
        away = lax.div(step + 1, 2)
        shift = away * (1 - 2 * lax.rem(step, 2))
        other = lax.rem(level + 12 + shift, DEPTH)
        for a, b in plane + [(side, py)]:
            send_row(a, other, b)

    for a, b in plane:
        send_row(a, level, b)

    whole = row_in.at[pl.ds(0, EXTENT - 1)]
    gone = slab_out.at[pl.ds(0, PLANE - 1), pl.ds(0, SLAB)]
    pltpu.make_async_copy(gone, gone, slab_s).wait()
    pltpu.make_async_copy(landed, landed, sum_s).wait()
    pltpu.make_async_copy(whole, whole, row_s).wait()
    pltpu.make_async_copy(whole, whole, row_r).wait()
    rows = row_in[...]
    sums = jnp.sum(rows, axis=0, keepdims=True)
    values = rows.T[MAPLANE : MAPLANE + 8]
    pair = jnp.concatenate([values, quarter_phase(values)], 1)
    final = dot3_few(pair, back_pair)
    maps_ref[...] = final
    sums = jnp.broadcast_to(sums, (8, 128))
    first_power = pltpu.roll(sums, 128 - NSHELL, 1)
    second_power = pltpu.roll(sums, 128 - 2 * NSHELL, 1)
    fsc_ref[...] = sums / (jnp.sqrt(first_power * second_power) + 1e-06)


def finish(final, shells, maps_ref, fsc_ref):
    for h in range(2):
        for c in range(2):
            for z in range(2):
                n = h * 4 + c * 2 + z
                maps_ref[h, c, z] = final[n : n + 1]
    fsc_ref[...] = shells[0, :NSHELL]


def shards(particles, orientation, wedge_index, half_set, shell_map):
    first, second, back, spread = tables()
    first, second, back = (halves(t) for t in (first, second, back))
    spread = jnp.asarray(spread, bf16)
    vmem = pl.BlockSpec(memory_space=pltpu.VMEM)
    hbm = pl.BlockSpec(memory_space=pltpu.HBM)
    dma = pltpu.SemaphoreType.DMA
    final, shells = pl.pallas_call(
        body,
        out_shape=(
            pltpu.VMEM((8, EXTENT), f32),
            pltpu.VMEM((8, 128), f32),
        ),
        in_specs=[hbm] * 9,
        out_specs=(vmem, vmem),
        scratch_shapes=[
            pltpu.SMEM((1,), jnp.int32), pltpu.SMEM((1,), jnp.int32), pltpu.SMEM((1,), jnp.int32),
            pltpu.VMEM((2, 2, BOX, BOX), f32),
            pltpu.VMEM((2, 1, EXTENT), jnp.int32),
            pltpu.VMEM((2, EXTENT, EXTENT), bf16),
            pltpu.VMEM((2, EXTENT, 2 * EXTENT), bf16),
            pltpu.VMEM((2, 2 * EXTENT, EXTENT), bf16),
            pltpu.VMEM((128, 2 * EXTENT), bf16),
            pltpu.VMEM((PLANE, SLAB + 7, 128), f32),
            pltpu.VMEM((PLANE, SLAB + 7, 128), f32),
            pltpu.VMEM((DEPTH, SUMS + 7, 128), f32),
            pltpu.VMEM((DEPTH, SUMS + 7, 128), f32),
            pltpu.VMEM((EXTENT, 128), f32),
            pltpu.VMEM((EXTENT, 128), f32),
            pltpu.VMEM((128, EXTENT), bf16),
            pltpu.VMEM((2, 128, EXTENT), bf16),
            dma((9,)),
            dma, dma((len(GROUPS),)), dma, dma, dma, dma,
            pltpu.SemaphoreType.REGULAR((3,)), pltpu.SemaphoreType.REGULAR((2,)),
        ],
        compiler_params=pltpu.CompilerParams(
            collective_id=0, has_side_effects=True,
        ),
        name="subtomogram_average",
    )(
        orientation, wedge_index, half_set, particles[0], shell_map, first, second, back, spread
    )
    final = pltpu.with_memory_space_constraint(final, pltpu.VMEM)
    shells = pltpu.with_memory_space_constraint(shells, pltpu.VMEM)
    return pl.pallas_call(
        finish,
        out_shape=(
            jax.ShapeDtypeStruct((2, 2, 2, 1, EXTENT), f32),
            jax.ShapeDtypeStruct((NSHELL,), f32),
        ),
        in_specs=[vmem, vmem],
        out_specs=(vmem, vmem),
        name="hand_out",
    )(final, shells)


def solution(mesh):
    both = ("px", "py")
    return jax.shard_map(
        shards,
        mesh=mesh,
        in_specs=(P(both, None, None, None, None), P(both), P(both), P(both), P(None, both, None)),
        out_specs=(P(None, None, None, both, None), P()),
        check_vma=False,
    )
```
